256 devices in a mesh: row: 16 (over y, x), col: 8 (over z), rep: 2 (over core).
Axes of the slice: x: 4, y: 4, z: 8, core: 2. Of those that a mesh axis runs over, the one named last changes fastest.
Arguments:
- patches: bfloat16 [2, 512, 6144], P('rep', 'col', 'row'), may hold values from -6 to 6
- cotangent: bfloat16 [2, 512, 6144], P('rep', 'col', 'row'), may hold values from -6 to 6
- w_in: bfloat16 [6144, 24576], P('row', 'col'), may hold values from -0.078125 to 0.078125
- w_out: bfloat16 [24576, 6144], P('col', 'row'), may hold values from -0.0390625 to 0.0390625
- moment_in: bfloat16 [2, 6144, 24576], P('rep', 'row', 'col'), may hold values from -2 to 2
- moment_out: bfloat16 [2, 24576, 6144], P('rep', 'col', 'row'), may hold values from -2 to 2
Outputs:
- mixed: bfloat16 [2, 512, 6144], P('rep', 'col', 'row')
- tally_in: bfloat16 [6144, 24576], P('row', 'col')
- tally_out: bfloat16 [24576, 6144], P('col', 'row')
The draws below stay inside these ranges and needn't reach their ends.
All inputs are finite; a program needn't handle non-finite values.
Results may differ from the reference program's by a relative error of at most 0.0055.
Values may be sent and summed in bfloat16 or wider, within the bound.
A program may use at most 128 MiB of HBM per device.

```python
import math
import jax
import jax.numpy as jnp
from jax import lax

D = 6144
FF = 24576
TOK_REP = 512
REPS = 2
N_REP = 2


def levels(key, extent, split, low, high):
    gain, own = 1.0, jax.random.fold_in(key, 6)
    for dim, parts in split:
        heights = jnp.exp(jax.random.uniform(jax.random.fold_in(own, dim), (parts,), jnp.float32, low / len(split), high / len(split)))
        gain = gain * jnp.repeat(heights, extent[dim] // parts).reshape([-1 if axis == dim else 1 for axis in range(len(extent))])
    return gain


def scatter_about(rng, dims, scale, reach, cuts=(), kind=jnp.bfloat16):
    values = scale * jax.random.normal(rng, dims, jnp.float32)
    if cuts:
        values = values * levels(rng, dims, cuts, -0.22, 0.18)
    return jnp.clip(values, -reach, reach).astype(kind)


def setup_inputs(seed: int = 0) -> dict:
    key_of = jax.random.split(jax.random.key(seed), 7)
    return {
        "patches": scatter_about(key_of[0], (REPS, TOK_REP, D), 1.0, 6.0, ((0, 2), (1, 8), (2, 16))),
        "cotangent": scatter_about(key_of[1], (REPS, TOK_REP, D), 1.0, 6.0, ((0, 2), (1, 8), (2, 16))),
        "w_in": scatter_about(key_of[2], (D, FF), D ** -0.5, 0.078125, ((0, 16), (1, 8))),
        "w_out": scatter_about(key_of[3], (FF, D), FF ** -0.5, 0.0390625, ((0, 8), (1, 16))),
        "moment_in": scatter_about(key_of[4], (REPS, D, FF), 0.3, 2.0, ((0, 2), (1, 16), (2, 8))),
        "moment_out": scatter_about(key_of[5], (REPS, FF, D), 0.3, 2.0, ((0, 2), (1, 8), (2, 16))),
    }


momentum_decay = 0.9
vote_scale = 0.3

def gelu_value(pre):
    return 0.5 * pre * (1.0 + lax.erf(pre * (1.0 / math.sqrt(2.0))))

def gelu_slope(pre):
    return 0.5 * (1.0 + lax.erf(pre * (1.0 / math.sqrt(2.0)))) + pre * jnp.exp(-0.5 * pre * pre) * (1.0 / math.sqrt(2.0 * math.pi))

def reference(patches, cotangent, w_in, w_out, moment_in, moment_out):
    norm_factor = 1.0 / math.sqrt(TOK_REP)
    tally_first = jnp.zeros((D, FF), jnp.float32)
    tally_second = jnp.zeros((FF, D), jnp.float32)
    outputs = []
    for replica in range(N_REP):
        inputs = patches[replica]
        grads = cotangent[replica]
        pre = jnp.dot(inputs, w_in, preferred_element_type=jnp.float32)
        hidden = gelu_value(pre).astype(jnp.bfloat16)
        outputs.append(jnp.dot(hidden, w_out, preferred_element_type=jnp.float32).astype(jnp.bfloat16))
        back = lax.dot_general(grads, w_out, (((1,), (1,)), ((), ())), preferred_element_type=jnp.float32)
        slope = (back * gelu_slope(pre)).astype(jnp.bfloat16)
        grad_first = lax.dot_general(inputs, slope, (((0,), (0,)), ((), ())), preferred_element_type=jnp.float32) * norm_factor
        grad_second = lax.dot_general(hidden, grads, (((0,), (0,)), ((), ())), preferred_element_type=jnp.float32) * norm_factor
        moved_first = momentum_decay * moment_in[replica].astype(jnp.float32) + (1.0 - momentum_decay) * grad_first
        moved_second = momentum_decay * moment_out[replica].astype(jnp.float32) + (1.0 - momentum_decay) * grad_second
        tally_first = tally_first + jnp.tanh(moved_first / vote_scale).astype(jnp.bfloat16).astype(jnp.float32)
        tally_second = tally_second + jnp.tanh(moved_second / vote_scale).astype(jnp.bfloat16).astype(jnp.float32)
    mixed = jnp.stack(outputs, axis=0)
    return (mixed, tally_first.astype(jnp.bfloat16), tally_second.astype(jnp.bfloat16))
```

```python
import math

import jax
import jax.numpy as jnp
from jax import lax
from jax.experimental import pallas as pl
from jax.experimental.pallas import tpu as pltpu
from jax.sharding import PartitionSpec as P

MESH = pl.DeviceIdType.MESH
BF16, F32 = jnp.bfloat16, jnp.float32

momentum_decay = 0.9
vote_scale = 0.3

BLOCKS, TOKENS, FEATURES, PIECES, WIDTH = 8, 64, 384, 8, 384
UNITS = 2 * BLOCKS
RING = 4
SUB = TOKENS // RING
STAGES = 9


def gelu_value(pre):
    return 0.5 * pre * (1.0 + lax.erf(pre * (1.0 / math.sqrt(2.0))))


def gelu_slope(pre):
    return 0.5 * (1.0 + lax.erf(pre * (1.0 / math.sqrt(2.0)))) + pre * jnp.exp(-0.5 * pre * pre) * (
        1.0 / math.sqrt(2.0 * math.pi)
    )


def token_offset(slot):
    return ((slot + 1) // 2) * ((slot % 2) * 2 - 1)


def step_kernel(
    pat_h, cot_h, win_h, wout_h, min_h, mout_h,
    mixed_o, tin_o, tout_o,
    xs, ws, mom, part, t1, r1, summed, t2, r2, pre_s, act, pat_t,
    mpart, mrecv, mown, mout_v, votes, vrecv,
    ld, ost, zsend, zrecv, rsend, rrecv, asend, arecv, msend, mrcv, vsend, vrcv,
):
    row, col, rep = lax.axis_index("row"), lax.axis_index("col"), lax.axis_index("rep")
    x, y = row % RING, row // RING
    a = x * (1 - rep) + y * rep
    b = y * (1 - rep) + x * rep

    def peer(a_to, b_to):
        x_to = a_to * (1 - rep) + b_to * rep
        y_to = b_to * (1 - rep) + a_to * rep
        return (y_to * RING + x_to, col, rep)

    ap, am, a2 = (a + 1) % RING, (a + 3) % RING, (a + 2) % RING
    bp, bm, b2 = (b + 1) % RING, (b + 3) % RING, (b + 2) % RING
    to_ap, to_am, to_bp, to_bm = peer(ap, b), peer(am, b), peer(a, bp), peer(a, bm)
    partner = (row, col, 1 - rep)

    def send(src, dst, send_sem, recv_sem, device):
        copy = pltpu.make_async_remote_copy(
            src_ref=src, dst_ref=dst, send_sem=send_sem, recv_sem=recv_sem,
            device_id=device, device_id_type=MESH,
        )
        copy.start()

    def arrived(ref, sem):
        pltpu.make_async_remote_copy(
            src_ref=ref, dst_ref=ref, send_sem=sem, recv_sem=sem, device_id=partner, device_id_type=MESH
        ).wait_recv()

    def departed(ref, sem):
        pltpu.make_async_remote_copy(
            src_ref=ref, dst_ref=ref, send_sem=sem, recv_sem=sem, device_id=partner, device_id_type=MESH
        ).wait_send()

    load_x = [
        pltpu.make_async_copy(pat_h.at[0], xs.at[0], ld.at[0]),
        pltpu.make_async_copy(cot_h.at[0], xs.at[BLOCKS], ld.at[1]),
    ]
    load_win = [
        pltpu.make_async_copy(win_h.at[:, pl.ds(p * WIDTH, WIDTH)], ws.at[p], ld.at[4 + p]) for p in range(PIECES)
    ]
    load_wout = pltpu.make_async_copy(wout_h, ws.at[pl.ds(PIECES, PIECES)], ld.at[2])
    load_mout = pltpu.make_async_copy(mout_h, mom.at[pl.ds(PIECES, PIECES)], ld.at[3])
    load_min = [
        pltpu.make_async_copy(min_h.at[0, :, pl.ds(p * WIDTH, WIDTH)], mom.at[p], ld.at[4 + PIECES + p])
        for p in range(PIECES)
    ]
    for copy in load_x + load_win + [load_wout]:
        copy.start()

    barrier = pltpu.get_barrier_semaphore()
    peers = [to_ap, to_am, to_bp, to_bm, partner] + [(row, (col + d) % BLOCKS, rep) for d in range(1, BLOCKS)]
    for device in peers:
        pl.semaphore_signal(barrier, inc=1, device_id=device, device_id_type=MESH)
    for copy in load_x + load_win:
        copy.wait()
    pl.semaphore_wait(barrier, len(peers))

    for base in (0, BLOCKS):
        for slot in range(1, BLOCKS):
            target = (row, (col - token_offset(slot) + BLOCKS) % BLOCKS, rep)
            send(xs.at[base], xs.at[base + slot], zsend.at[base + slot], zrecv.at[base + slot], target)

    load_wout.wait()
    for copy in load_min + [load_mout]:
        copy.start()

    def reduce_start(q):
        @pl.when(q % BLOCKS != 0)
        def _():
            arrived(xs.at[q], zrecv.at[q])

        tokens = xs[q]

        @pl.when(q < BLOCKS)
        def _():
            for p in range(PIECES):
                part[q, p] = jnp.dot(tokens, ws[p], preferred_element_type=F32).astype(BF16)

        @pl.when(q >= BLOCKS)
        def _():
            for p in range(PIECES):
                part[q, p] = lax.dot_general(
                    tokens, ws[PIECES + p], (((1,), (1,)), ((), ())), preferred_element_type=F32
                ).astype(BF16)

        send(part.at[q, 2 * a2], t1.at[q, 0], rsend.at[0, q], rrecv.at[0, q], to_ap)
        send(part.at[q, 2 * a2 + 1], t1.at[q, 1], rsend.at[0, q], rrecv.at[0, q], to_am)
        send(part.at[q, 2 * ap + 1], r1.at[q, 1], rsend.at[0, q], rrecv.at[1, q], to_ap)
        send(part.at[q, 2 * am], r1.at[q, 2], rsend.at[0, q], rrecv.at[1, q], to_am)

    def reduce_relay(q):
        arrived(t1.at[q], rrecv.at[0, q])
        part[q, 2 * ap] = (part[q, 2 * ap].astype(F32) + t1[q, 0].astype(F32)).astype(BF16)
        part[q, 2 * am + 1] = (part[q, 2 * am + 1].astype(F32) + t1[q, 1].astype(F32)).astype(BF16)
        send(part.at[q, 2 * ap], r1.at[q, 0], rsend.at[1, q], rrecv.at[1, q], to_ap)
        send(part.at[q, 2 * am + 1], r1.at[q, 3], rsend.at[1, q], rrecv.at[1, q], to_am)

    def second_start(q):
        arrived(r1.at[q], rrecv.at[1, q])
        for h in range(2):
            total = part[q, 2 * a + h].astype(F32) + r1[q, h].astype(F32) + r1[q, 2 + h].astype(F32)
            summed[q, h] = total.astype(BF16).reshape(RING, SUB, WIDTH)
        send(summed.at[q, 0, b2], t2.at[q, 0], rsend.at[2, q], rrecv.at[2, q], to_bp)
        send(summed.at[q, 1, b2], t2.at[q, 1], rsend.at[2, q], rrecv.at[2, q], to_bm)
        send(summed.at[q, 1, bp], r2.at[q, 1], rsend.at[2, q], rrecv.at[3, q], to_bp)
        send(summed.at[q, 0, bm], r2.at[q, 2], rsend.at[2, q], rrecv.at[3, q], to_bm)

    def second_relay(q):
        arrived(t2.at[q], rrecv.at[2, q])
        summed[q, 0, bp] = (summed[q, 0, bp].astype(F32) + t2[q, 0].astype(F32)).astype(BF16)
        summed[q, 1, bm] = (summed[q, 1, bm].astype(F32) + t2[q, 1].astype(F32)).astype(BF16)
        send(summed.at[q, 0, bp], r2.at[q, 0], rsend.at[3, q], rrecv.at[3, q], to_bp)
        send(summed.at[q, 1, bm], r2.at[q, 3], rsend.at[3, q], rrecv.at[3, q], to_bm)

    def activate(q):
        arrived(r2.at[q], rrecv.at[3, q])
        totals = [
            summed[q, h, b].astype(F32) + r2[q, h].astype(F32) + r2[q, 2 + h].astype(F32) for h in range(2)
        ]

        @pl.when(q < BLOCKS)
        def _():
            for h in range(2):
                pre_s[q, h] = totals[h]
                act[q, 2 * a + h, b] = gelu_value(totals[h]).astype(BF16)

        @pl.when(q >= BLOCKS)
        def _():
            for h in range(2):
                slope = gelu_slope(pre_s[q - BLOCKS, h])
                act[q, 2 * a + h, b] = (totals[h] * slope).astype(BF16)

        mine = act.at[q, pl.ds(2 * a, 2), b]
        send(mine, mine, asend.at[0, q], arecv.at[0, q], to_bp)
        send(mine, mine, asend.at[0, q], arecv.at[0, q], to_bm)

    def second_spread(q):
        arrived(part.at[q, 0], arecv.at[0, q])
        ahead, behind = act.at[q, 2 * a, bm], act.at[q, 2 * a + 1, bp]
        send(ahead, ahead, asend.at[1, q], arecv.at[1, q], to_bp)
        send(behind, behind, asend.at[1, q], arecv.at[1, q], to_bm)

    def first_spread(q):
        arrived(t2.at[q], arecv.at[1, q])
        mine = act.at[q, pl.ds(2 * a, 2)]
        send(mine, mine, asend.at[2, q], arecv.at[2, q], to_ap)
        send(mine, mine, asend.at[2, q], arecv.at[2, q], to_am)

    def first_relay(q):
        arrived(r1.at[q], arecv.at[2, q])
        ahead, behind = act.at[q, 2 * am], act.at[q, 2 * ap + 1]
        send(ahead, ahead, asend.at[3, q], arecv.at[3, q], to_ap)
        send(behind, behind, asend.at[3, q], arecv.at[3, q], to_am)

    def complete(q):
        arrived(t1.at[q], arecv.at[3, q])

        @pl.when(q < BLOCKS)
        def _():
            total = jnp.zeros((TOKENS, FEATURES), F32)
            for p in range(PIECES):
                total += jnp.dot(
                    act[q, p].reshape(TOKENS, WIDTH), ws[PIECES + p], preferred_element_type=F32
                )

            @pl.when(q == 0)
            def _():
                mown[...] = total

            @pl.when(q > 0)
            def _():
                mpart[q] = total.astype(BF16)
                target = (row, (col + token_offset(q) + BLOCKS) % BLOCKS, rep)
                send(mpart.at[q], mrecv.at[q], msend.at[q], mrcv.at[q], target)

    grad_factor = (1.0 - momentum_decay) / vote_scale / math.sqrt(BLOCKS * TOKENS)
    moment_factor = momentum_decay / vote_scale

    def vote(grad, index):
        moved = moment_factor * mom[index].astype(F32) + grad_factor * grad
        votes[index] = jnp.tanh(moved).astype(BF16)
        send(votes.at[index], vrecv.at[index], vsend.at[index], vrcv.at[index], partner)

    def vote_second(p):
        hidden = act[pl.ds(0, BLOCKS), p].reshape(BLOCKS * TOKENS, WIDTH)
        cotangent = xs[pl.ds(BLOCKS, BLOCKS)].reshape(BLOCKS * TOKENS, FEATURES)
        grad = lax.dot_general(hidden, cotangent, (((0,), (0,)), ((), ())), preferred_element_type=F32)
        vote(grad, PIECES + p)

    def vote_first(p):
        slope = act[pl.ds(BLOCKS, BLOCKS), p].reshape(BLOCKS * TOKENS, WIDTH)
        grad = jnp.dot(pat_t[...], slope, preferred_element_type=F32)
        vote(grad, p)

    def tally(index):
        arrived(vrecv.at[index], vrcv.at[index])
        vrecv[index] = (votes[index].astype(F32) + vrecv[index].astype(F32)).astype(BF16)

    stages = (
        reduce_start, reduce_relay, second_start, second_relay, activate,
        second_spread, first_spread, first_relay, complete,
    )

    def turn(i, carry):
        for lag, stage in enumerate(stages):

            @pl.when((i >= lag) & (i < UNITS + lag))
            def _(lag=lag, stage=stage):
                stage(i - lag)

        @pl.when(i == UNITS)
        def _():
            load_mout.wait()
            pat_t[...] = xs[pl.ds(0, BLOCKS)].reshape(BLOCKS * TOKENS, FEATURES).T

        @pl.when(i >= UNITS)
        def _():
            vote_second(i - UNITS)

        return carry

    lax.fori_loop(0, UNITS + STAGES - 1, turn, 0)

    for copy in load_min:
        copy.wait()

    def first_turn(p, carry):
        vote_first(p)
        return carry

    lax.fori_loop(0, PIECES, first_turn, 0)

    def second_out(p, carry):
        tally(PIECES + p)
        pltpu.make_async_copy(vrecv.at[PIECES + p], tout_o.at[p], ost.at[PIECES + p]).start()
        return carry

    lax.fori_loop(0, PIECES, second_out, 0)

    total = mown[...]
    for slot in range(1, BLOCKS):
        arrived(mrecv.at[slot], mrcv.at[slot])
        total += mrecv[slot].astype(F32)
    mout_v[...] = total.astype(BF16)
    store_mixed = pltpu.make_async_copy(mout_v, mixed_o.at[0], ld.at[0])
    store_mixed.start()

    for p in range(PIECES):
        tally(p)
        pltpu.make_async_copy(vrecv.at[p], tin_o.at[:, pl.ds(p * WIDTH, WIDTH)], ost.at[p]).start()

    def drain(q, carry):
        departed(part.at[q, pl.ds(0, 4)], rsend.at[0, q])
        departed(part.at[q, pl.ds(0, 2)], rsend.at[1, q])
        departed(summed.at[q, 0], rsend.at[2, q])
        departed(t2.at[q], rsend.at[3, q])
        departed(summed.at[q, 0], asend.at[0, q])
        departed(t2.at[q], asend.at[1, q])
        departed(part.at[q, pl.ds(0, 4)], asend.at[2, q])
        departed(part.at[q, pl.ds(0, 2)], asend.at[3, q])
        departed(votes.at[q], vsend.at[q])

        @pl.when(q % BLOCKS != 0)
        def _():
            departed(xs.at[q], zsend.at[q])

        return carry

    lax.fori_loop(0, UNITS, drain, 0)
    for slot in range(1, BLOCKS):
        departed(mpart.at[slot], msend.at[slot])
    store_mixed.wait()
    for p in range(PIECES):
        pltpu.make_async_copy(vrecv.at[PIECES + p], tout_o.at[p], ost.at[PIECES + p]).wait()
        pltpu.make_async_copy(vrecv.at[p], tin_o.at[:, pl.ds(p * WIDTH, WIDTH)], ost.at[p]).wait()


def shards(patches, cotangent, w_in, w_out, moment_in, moment_out):
    by_piece = (PIECES, WIDTH, FEATURES)
    anywhere = pl.BlockSpec(memory_space=pl.ANY)
    mixed, tally_first, tally_second = pl.pallas_call(
        step_kernel,
        out_shape=(
            jax.ShapeDtypeStruct((1, TOKENS, FEATURES), BF16),
            jax.ShapeDtypeStruct((FEATURES, PIECES * WIDTH), BF16),
            jax.ShapeDtypeStruct(by_piece, BF16),
        ),
        in_specs=[anywhere] * 6,
        out_specs=(anywhere,) * 3,
        scratch_shapes=[
            pltpu.VMEM((UNITS, TOKENS, FEATURES), BF16),
            pltpu.VMEM((UNITS, WIDTH, FEATURES), BF16),
            pltpu.VMEM((UNITS, WIDTH, FEATURES), BF16),
            pltpu.VMEM((UNITS, PIECES, TOKENS, WIDTH), BF16),
            pltpu.VMEM((UNITS, 2, TOKENS, WIDTH), BF16),
            pltpu.VMEM((UNITS, 4, TOKENS, WIDTH), BF16),
            pltpu.VMEM((UNITS, 2, RING, SUB, WIDTH), BF16),
            pltpu.VMEM((UNITS, 2, SUB, WIDTH), BF16),
            pltpu.VMEM((UNITS, 4, SUB, WIDTH), BF16),
            pltpu.VMEM((BLOCKS, 2, SUB, WIDTH), F32),
            pltpu.VMEM((UNITS, PIECES, RING, SUB, WIDTH), BF16),
            pltpu.VMEM((FEATURES, BLOCKS * TOKENS), BF16),
            pltpu.VMEM((BLOCKS, TOKENS, FEATURES), BF16),
            pltpu.VMEM((BLOCKS, TOKENS, FEATURES), BF16),
            pltpu.VMEM((TOKENS, FEATURES), F32),
            pltpu.VMEM((TOKENS, FEATURES), BF16),
            pltpu.VMEM((UNITS, WIDTH, FEATURES), BF16),
            pltpu.VMEM((UNITS, WIDTH, FEATURES), BF16),
            pltpu.SemaphoreType.DMA((4 + 2 * PIECES,)),
            pltpu.SemaphoreType.DMA((UNITS,)),
            pltpu.SemaphoreType.DMA((UNITS,)),
            pltpu.SemaphoreType.DMA((UNITS,)),
            pltpu.SemaphoreType.DMA((4, UNITS)),
            pltpu.SemaphoreType.DMA((4, UNITS)),
            pltpu.SemaphoreType.DMA((4, UNITS)),
            pltpu.SemaphoreType.DMA((4, UNITS)),
            pltpu.SemaphoreType.DMA((BLOCKS,)),
            pltpu.SemaphoreType.DMA((BLOCKS,)),
            pltpu.SemaphoreType.DMA((UNITS,)),
            pltpu.SemaphoreType.DMA((UNITS,)),
        ],
        compiler_params=pltpu.CompilerParams(
            collective_id=0, has_side_effects=True, vmem_limit_bytes=60 * 1024 * 1024
        ),
    )(
        patches, cotangent, w_in, w_out.reshape(by_piece), moment_in, moment_out[0].reshape(by_piece),
    )
    return mixed, tally_first, tally_second.reshape(PIECES * WIDTH, FEATURES)


def solution(mesh):
    in_specs = (
        P("rep", "col", "row"),
        P("rep", "col", "row"),
        P("row", "col"),
        P("col", "row"),
        P("rep", "row", "col"),
        P("rep", "col", "row"),
    )
    out_specs = (P("rep", "col", "row"), P("row", "col"), P("col", "row"))
    return jax.shard_map(shards, mesh=mesh, in_specs=in_specs, out_specs=out_specs, check_vma=False)
```

```python
import math

import jax
import jax.numpy as jnp
from jax import lax
from jax.experimental import pallas as pl
from jax.experimental.pallas import tpu as pltpu
from jax.sharding import PartitionSpec as P

MESH = pl.DeviceIdType.MESH
BF16, F32 = jnp.bfloat16, jnp.float32

momentum_decay = 0.9
vote_scale = 0.3

BLOCKS, TOKENS, FEATURES, PIECES, WIDTH = 8, 64, 384, 8, 384
UNITS = 2 * BLOCKS
RING = 4
SUB = TOKENS // RING
STAGES, LAG = 9, 2
VMEM_LIMIT = 52 * 1024 * 1024
TURNS = UNITS + LAG * (STAGES - 1)


def gelu_value(pre):
    return 0.5 * pre * (1.0 + lax.erf(pre * (1.0 / math.sqrt(2.0))))


def gelu_slope(pre):
    return 0.5 * (1.0 + lax.erf(pre * (1.0 / math.sqrt(2.0)))) + pre * jnp.exp(-0.5 * pre * pre) * (
        1.0 / math.sqrt(2.0 * math.pi)
    )


def token_offset(slot):
    return ((slot + 1) // 2) * ((slot % 2) * 2 - 1)


def step_kernel(
    pat_h, cot_h, win_h, wout_h, min_h, mout_h,
    mixed_v, tallies,
    xs, ws, mom, part, own, t1, r1, summed, total_s, t2, r2, pre_s, act, pat_t,
    mpart, mrecv, votes,
    ld, zsend, zrecv, rsend, rrecv, asend, arecv, msend, mrcv, vsend, vrcv,
):
    row, col, rep = lax.axis_index("row"), lax.axis_index("col"), lax.axis_index("rep")
    x, y = row % RING, row // RING
    a = x * (1 - rep) + y * rep
    b = y * (1 - rep) + x * rep

    def peer(a_to, b_to):
        x_to = a_to * (1 - rep) + b_to * rep
        y_to = b_to * (1 - rep) + a_to * rep
        return (y_to * RING + x_to, col, rep)

    ap, am, a2 = (a + 1) % RING, (a + 3) % RING, (a + 2) % RING
    bp, bm, b2 = (b + 1) % RING, (b + 3) % RING, (b + 2) % RING
    to_ap, to_am, to_bp, to_bm = peer(ap, b), peer(am, b), peer(a, bp), peer(a, bm)
    partner = (row, col, 1 - rep)

    def send(src, dst, send_sem, recv_sem, device):
        copy = pltpu.make_async_remote_copy(
            src_ref=src, dst_ref=dst, send_sem=send_sem, recv_sem=recv_sem,
            device_id=device, device_id_type=MESH,
        )
        copy.start()

    def arrived(ref, sem):
        pltpu.make_async_remote_copy(
            src_ref=ref, dst_ref=ref, send_sem=sem, recv_sem=sem, device_id=partner, device_id_type=MESH
        ).wait_recv()

    def departed(ref, sem):
        pltpu.make_async_remote_copy(
            src_ref=ref, dst_ref=ref, send_sem=sem, recv_sem=sem, device_id=partner, device_id_type=MESH
        ).wait_send()

    load_x = [
        pltpu.make_async_copy(pat_h.at[0], xs.at[0], ld.at[0]),
        pltpu.make_async_copy(cot_h.at[0], xs.at[BLOCKS], ld.at[1]),
    ]
    load_win = [
        pltpu.make_async_copy(win_h.at[:, pl.ds(p * WIDTH, WIDTH)], ws.at[p], ld.at[4 + p]) for p in range(PIECES)
    ]
    load_wout = pltpu.make_async_copy(wout_h, ws.at[pl.ds(PIECES, PIECES)], ld.at[2])
    load_mout = pltpu.make_async_copy(mout_h, mom.at[pl.ds(PIECES, PIECES)], ld.at[3])
    load_min = [
        pltpu.make_async_copy(min_h.at[0, :, pl.ds(p * WIDTH, WIDTH)], mom.at[p], ld.at[4 + PIECES + p])
        for p in range(PIECES)
    ]
    for copy in load_x + load_win + [load_wout]:
        copy.start()

    barrier = pltpu.get_barrier_semaphore()
    peers = [to_ap, to_am, to_bp, to_bm, partner] + [(row, (col + d) % BLOCKS, rep) for d in range(1, BLOCKS)]
    for device in peers:
        pl.semaphore_signal(barrier, inc=1, device_id=device, device_id_type=MESH)
    for copy in load_x + load_win:
        copy.wait()
    pl.semaphore_wait(barrier, len(peers))

    for base in (0, BLOCKS):
        for slot in range(1, BLOCKS):
            target = (row, (col - token_offset(slot) + BLOCKS) % BLOCKS, rep)
            send(xs.at[base], xs.at[base + slot], zsend.at[base + slot], zrecv.at[base + slot], target)

    load_wout.wait()
    for copy in load_min + [load_mout]:
        copy.start()

    def reduce_start(q):
        @pl.when(q % BLOCKS != 0)
        def _():
            arrived(xs.at[q], zrecv.at[q])

        tokens = xs[q]

        def piece(p):
            return jnp.dot(tokens, ws[p], preferred_element_type=F32)

        def piece_back(p):
            return lax.dot_general(
                tokens, ws[PIECES + p], (((1,), (1,)), ((), ())), preferred_element_type=F32
            )

        def products(term):
            for block in (a2, ap, am):
                for h in range(2):
                    part[q, 2 * block + h] = term(2 * block + h).astype(BF16)
            for h in range(2):
                own[q, h] = term(2 * a + h)

        @pl.when(q < BLOCKS)
        def _():
            products(piece)

        @pl.when(q >= BLOCKS)
        def _():
            products(piece_back)

        send(part.at[q, 2 * a2], t1.at[q, 0], rsend.at[0, q], rrecv.at[0, q], to_ap)
        send(part.at[q, 2 * a2 + 1], t1.at[q, 1], rsend.at[0, q], rrecv.at[0, q], to_am)
        send(part.at[q, 2 * ap + 1], r1.at[q, 1], rsend.at[0, q], rrecv.at[1, q], to_ap)
        send(part.at[q, 2 * am], r1.at[q, 2], rsend.at[0, q], rrecv.at[1, q], to_am)

    def reduce_relay(q):
        arrived(t1.at[q], rrecv.at[0, q])
        part[q, 2 * ap] = (part[q, 2 * ap].astype(F32) + t1[q, 0].astype(F32)).astype(BF16)
        part[q, 2 * am + 1] = (part[q, 2 * am + 1].astype(F32) + t1[q, 1].astype(F32)).astype(BF16)
        send(part.at[q, 2 * ap], r1.at[q, 0], rsend.at[1, q], rrecv.at[1, q], to_ap)
        send(part.at[q, 2 * am + 1], r1.at[q, 3], rsend.at[1, q], rrecv.at[1, q], to_am)

    def second_start(q):
        arrived(r1.at[q], rrecv.at[1, q])
        for h in range(2):
            total = own[q, h] + r1[q, h].astype(F32) + r1[q, 2 + h].astype(F32)
            total = total.reshape(RING, SUB, WIDTH)
            total_s[q, h] = total
            summed[q, h] = total.astype(BF16)
        send(summed.at[q, 0, b2], t2.at[q, 0], rsend.at[2, q], rrecv.at[2, q], to_bp)
        send(summed.at[q, 1, b2], t2.at[q, 1], rsend.at[2, q], rrecv.at[2, q], to_bm)
        send(summed.at[q, 1, bp], r2.at[q, 1], rsend.at[2, q], rrecv.at[3, q], to_bp)
        send(summed.at[q, 0, bm], r2.at[q, 2], rsend.at[2, q], rrecv.at[3, q], to_bm)

    def second_relay(q):
        arrived(t2.at[q], rrecv.at[2, q])
        summed[q, 0, bp] = (summed[q, 0, bp].astype(F32) + t2[q, 0].astype(F32)).astype(BF16)
        summed[q, 1, bm] = (summed[q, 1, bm].astype(F32) + t2[q, 1].astype(F32)).astype(BF16)
        send(summed.at[q, 0, bp], r2.at[q, 0], rsend.at[3, q], rrecv.at[3, q], to_bp)
        send(summed.at[q, 1, bm], r2.at[q, 3], rsend.at[3, q], rrecv.at[3, q], to_bm)

    def activate(q):
        arrived(r2.at[q], rrecv.at[3, q])
        totals = [
            total_s[q, h, b] + r2[q, h].astype(F32) + r2[q, 2 + h].astype(F32) for h in range(2)
        ]

        @pl.when(q < BLOCKS)
        def _():
            for h in range(2):
                pre_s[q, h] = totals[h]
                act[q, 2 * a + h, b] = gelu_value(totals[h]).astype(BF16)

        @pl.when(q >= BLOCKS)
        def _():
            for h in range(2):
                slope = gelu_slope(pre_s[q - BLOCKS, h])
                act[q, 2 * a + h, b] = (totals[h] * slope).astype(BF16)

        mine = act.at[q, pl.ds(2 * a, 2), b]
        send(mine, mine, asend.at[0, q], arecv.at[0, q], to_bp)
        send(mine, mine, asend.at[0, q], arecv.at[0, q], to_bm)

    def second_spread(q):
        arrived(part.at[q, 0], arecv.at[0, q])
        ahead, behind = act.at[q, 2 * a, bm], act.at[q, 2 * a + 1, bp]
        send(ahead, ahead, asend.at[1, q], arecv.at[1, q], to_bp)
        send(behind, behind, asend.at[1, q], arecv.at[1, q], to_bm)

    def first_spread(q):
        arrived(t2.at[q], arecv.at[1, q])
        mine = act.at[q, pl.ds(2 * a, 2)]
        send(mine, mine, asend.at[2, q], arecv.at[2, q], to_ap)
        send(mine, mine, asend.at[2, q], arecv.at[2, q], to_am)

    def first_relay(q):
        arrived(r1.at[q], arecv.at[2, q])
        ahead, behind = act.at[q, 2 * am], act.at[q, 2 * ap + 1]
        send(ahead, ahead, asend.at[3, q], arecv.at[3, q], to_ap)
        send(behind, behind, asend.at[3, q], arecv.at[3, q], to_am)

    def complete(q):
        arrived(t1.at[q], arecv.at[3, q])

        @pl.when(q < BLOCKS)
        def _():
            total = jnp.zeros((TOKENS, FEATURES), F32)
            for p in range(PIECES):
                total += jnp.dot(
                    act[q, p].reshape(TOKENS, WIDTH), ws[PIECES + p], preferred_element_type=F32
                )

            mpart[q] = total

            @pl.when(q > 0)
            def _():
                target = (row, (col + token_offset(q) + BLOCKS) % BLOCKS, rep)
                send(mpart.at[q], mrecv.at[q], msend.at[q], mrcv.at[q], target)

    grad_factor = (1.0 - momentum_decay) / vote_scale / math.sqrt(BLOCKS * TOKENS)
    moment_factor = momentum_decay / vote_scale

    def vote(grad, index):
        moved = moment_factor * mom[index].astype(F32) + grad_factor * grad
        votes[index] = jnp.tanh(moved).astype(BF16)
        send(votes.at[index], tallies.at[index], vsend.at[index], vrcv.at[index], partner)

    def vote_second(p):
        hidden = act[pl.ds(0, BLOCKS), p].reshape(BLOCKS * TOKENS, WIDTH)
        cotangent = xs[pl.ds(BLOCKS, BLOCKS)].reshape(BLOCKS * TOKENS, FEATURES)
        grad = lax.dot_general(hidden, cotangent, (((0,), (0,)), ((), ())), preferred_element_type=F32)
        vote(grad, PIECES + p)

    def vote_first(p):
        slope = act[pl.ds(BLOCKS, BLOCKS), p].reshape(BLOCKS * TOKENS, WIDTH)
        grad = jnp.dot(pat_t[...], slope, preferred_element_type=F32)
        vote(grad, p)

    def tally(index):
        arrived(tallies.at[index], vrcv.at[index])
        tallies[index] = (votes[index].astype(F32) + tallies[index].astype(F32)).astype(BF16)

    stages = (
        reduce_start, reduce_relay, second_start, second_relay, activate,
        second_spread, first_spread, first_relay, complete,
    )

    def turn(i, carry):
        for place, stage in enumerate(stages):
            lag = LAG * place

            @pl.when((i >= lag) & (i < UNITS + lag))
            def _(lag=lag, stage=stage):
                stage(i - lag)

        @pl.when(i == TURNS - BLOCKS)
        def _():
            load_mout.wait()
            pat_t[...] = xs[pl.ds(0, BLOCKS)].reshape(BLOCKS * TOKENS, FEATURES).T

        @pl.when(i >= TURNS - BLOCKS)
        def _():
            vote_second(i - (TURNS - BLOCKS))

        return carry

    lax.fori_loop(0, TURNS, turn, 0)

    for copy in load_min:
        copy.wait()

    def first_turn(p, carry):
        vote_first(p)
        return carry

    lax.fori_loop(0, PIECES, first_turn, 0)

    def second_tally(p, carry):
        tally(PIECES + p)
        return carry

    lax.fori_loop(0, PIECES, second_tally, 0)

    total = mpart[0]
    for slot in range(1, BLOCKS):
        arrived(mrecv.at[slot], mrcv.at[slot])
        total += mrecv[slot]
    mixed_v[...] = total.astype(BF16)

    def first_tally(p, carry):
        tally(p)
        return carry

    lax.fori_loop(0, PIECES, first_tally, 0)

    def drain(q, carry):
        departed(part.at[q, pl.ds(0, 4)], rsend.at[0, q])
        departed(part.at[q, pl.ds(0, 2)], rsend.at[1, q])
        departed(summed.at[q, 0], rsend.at[2, q])
        departed(t2.at[q], rsend.at[3, q])
        departed(summed.at[q, 0], asend.at[0, q])
        departed(t2.at[q], asend.at[1, q])
        departed(part.at[q, pl.ds(0, 4)], asend.at[2, q])
        departed(part.at[q, pl.ds(0, 2)], asend.at[3, q])
        departed(votes.at[q], vsend.at[q])

        @pl.when(q % BLOCKS != 0)
        def _():
            departed(xs.at[q], zsend.at[q])

        return carry

    lax.fori_loop(0, UNITS, drain, 0)
    for slot in range(1, BLOCKS):
        departed(mpart.at[slot], msend.at[slot])


def output_kernel(mixed_v, tallies, mixed_o, tin_o, tout_o, sems):
    copies = [
        pltpu.make_async_copy(mixed_v, mixed_o.at[0], sems.at[0]),
        pltpu.make_async_copy(tallies.at[pl.ds(PIECES, PIECES)], tout_o, sems.at[1]),
    ]
    for p in range(PIECES):
        columns = tin_o.at[:, pl.ds(p * WIDTH, WIDTH)]
        copies.append(pltpu.make_async_copy(tallies.at[p], columns, sems.at[2 + p]))
    for copy in copies:
        copy.start()
    for copy in copies:
        copy.wait()


def shards(patches, cotangent, w_in, w_out, moment_in, moment_out):
    by_piece = (PIECES, WIDTH, FEATURES)
    anywhere = pl.BlockSpec(memory_space=pl.ANY)
    in_vmem = pl.BlockSpec(memory_space=pltpu.VMEM)
    results = pl.pallas_call(
        step_kernel,
        out_shape=(
            pltpu.VMEM((TOKENS, FEATURES), BF16),
            pltpu.VMEM((UNITS, WIDTH, FEATURES), BF16),
        ),
        in_specs=[anywhere] * 6,
        out_specs=(in_vmem,) * 2,
        scratch_shapes=[
            pltpu.VMEM((UNITS, TOKENS, FEATURES), BF16),
            pltpu.VMEM((UNITS, WIDTH, FEATURES), BF16),
            pltpu.VMEM((UNITS, WIDTH, FEATURES), BF16),
            pltpu.VMEM((UNITS, PIECES, TOKENS, WIDTH), BF16),
            pltpu.VMEM((UNITS, 2, TOKENS, WIDTH), F32),
            pltpu.VMEM((UNITS, 2, TOKENS, WIDTH), BF16),
            pltpu.VMEM((UNITS, 4, TOKENS, WIDTH), BF16),
            pltpu.VMEM((UNITS, 2, RING, SUB, WIDTH), BF16),
            pltpu.VMEM((UNITS, 2, RING, SUB, WIDTH), F32),
            pltpu.VMEM((UNITS, 2, SUB, WIDTH), BF16),
            pltpu.VMEM((UNITS, 4, SUB, WIDTH), BF16),
            pltpu.VMEM((BLOCKS, 2, SUB, WIDTH), F32),
            pltpu.VMEM((UNITS, PIECES, RING, SUB, WIDTH), BF16),
            pltpu.VMEM((FEATURES, BLOCKS * TOKENS), BF16),
            pltpu.VMEM((BLOCKS, TOKENS, FEATURES), F32),
            pltpu.VMEM((BLOCKS, TOKENS, FEATURES), F32),
            pltpu.VMEM((UNITS, WIDTH, FEATURES), BF16),
            pltpu.SemaphoreType.DMA((4 + 2 * PIECES,)),
            pltpu.SemaphoreType.DMA((UNITS,)),
            pltpu.SemaphoreType.DMA((UNITS,)),
            pltpu.SemaphoreType.DMA((4, UNITS)),
            pltpu.SemaphoreType.DMA((4, UNITS)),
            pltpu.SemaphoreType.DMA((4, UNITS)),
            pltpu.SemaphoreType.DMA((4, UNITS)),
            pltpu.SemaphoreType.DMA((BLOCKS,)),
            pltpu.SemaphoreType.DMA((BLOCKS,)),
            pltpu.SemaphoreType.DMA((UNITS,)),
            pltpu.SemaphoreType.DMA((UNITS,)),
        ],
        compiler_params=pltpu.CompilerParams(
            collective_id=0, has_side_effects=True, vmem_limit_bytes=VMEM_LIMIT
        ),
    )(
        patches, cotangent, w_in, w_out.reshape(by_piece), moment_in, moment_out[0].reshape(by_piece),
    )
    mixed, tally_first, tally_second = pl.pallas_call(
        output_kernel,
        out_shape=(
            jax.ShapeDtypeStruct((1, TOKENS, FEATURES), BF16),
            jax.ShapeDtypeStruct((FEATURES, PIECES * WIDTH), BF16),
            jax.ShapeDtypeStruct(by_piece, BF16),
        ),
        in_specs=[in_vmem] * 2,
        out_specs=(anywhere,) * 3,
        scratch_shapes=[pltpu.SemaphoreType.DMA((2 + PIECES,))],
        compiler_params=pltpu.CompilerParams(vmem_limit_bytes=2**20),
    )(*results)
    return mixed, tally_first, tally_second.reshape(PIECES * WIDTH, FEATURES)


def solution(mesh):
    in_specs = (
        P("rep", "col", "row"),
        P("rep", "col", "row"),
        P("row", "col"),
        P("col", "row"),
        P("rep", "row", "col"),
        P("rep", "col", "row"),
    )
    out_specs = (P("rep", "col", "row"), P("row", "col"), P("col", "row"))
    return jax.shard_map(shards, mesh=mesh, in_specs=in_specs, out_specs=out_specs, check_vma=False)
```

```python
import math

import jax
import jax.numpy as jnp
from jax import lax
from jax.experimental import pallas as pl
from jax.experimental.pallas import tpu as pltpu
from jax.sharding import PartitionSpec as P

MESH = pl.DeviceIdType.MESH
BF16, F32 = jnp.bfloat16, jnp.float32

momentum_decay = 0.9
vote_scale = 0.3

BLOCKS, TOKENS, FEATURES, PIECES, WIDTH = 8, 64, 384, 8, 384
UNITS = 2 * BLOCKS
RING = 4
SUB = TOKENS // RING
LAGS = (0, 2, 5, 7, 10, 12, 15, 19, 23)
VMEM_LIMIT = 52 * 1024 * 1024
TURNS = UNITS + LAGS[-1]
TALLY_TURNS = 5


def gelu_value(pre):
    return 0.5 * pre * (1.0 + lax.erf(pre * (1.0 / math.sqrt(2.0))))


def gelu_slope(pre):
    return 0.5 * (1.0 + lax.erf(pre * (1.0 / math.sqrt(2.0)))) + pre * jnp.exp(-0.5 * pre * pre) * (
        1.0 / math.sqrt(2.0 * math.pi)
    )


def unit_at(place):
    moved = jnp.where(place <= BLOCKS, place - 1, place)
    return jnp.where(place == 0, 0, jnp.where(place == 1, BLOCKS, moved))


def token_offset(slot):
    return ((slot + 1) // 2) * ((slot % 2) * 2 - 1)


def step_kernel(
    pat_h, cot_h, win_h, wout_h, min_h, mout_h,
    mixed_v, tallies,
    xs, ws, mom, part, own, t1, r1, summed, total_s, t2, r2, pre_s, act, pat_t, hid_t,
    mpart, mrecv, votes,
    ld, zsend, zrecv, rsend, rrecv, asend, arecv, msend, mrcv, vsend, vrcv,
):
    row, col, rep = lax.axis_index("row"), lax.axis_index("col"), lax.axis_index("rep")
    x, y = row % RING, row // RING
    a = x * (1 - rep) + y * rep
    b = y * (1 - rep) + x * rep

    def peer(a_to, b_to):
        x_to = a_to * (1 - rep) + b_to * rep
        y_to = b_to * (1 - rep) + a_to * rep
        return (y_to * RING + x_to, col, rep)

    ap, am, a2 = (a + 1) % RING, (a + 3) % RING, (a + 2) % RING
    bp, bm, b2 = (b + 1) % RING, (b + 3) % RING, (b + 2) % RING
    to_ap, to_am, to_bp, to_bm = peer(ap, b), peer(am, b), peer(a, bp), peer(a, bm)
    partner = (row, col, 1 - rep)

    def send(src, dst, send_sem, recv_sem, device):
        copy = pltpu.make_async_remote_copy(
            src_ref=src, dst_ref=dst, send_sem=send_sem, recv_sem=recv_sem,
            device_id=device, device_id_type=MESH,
        )
        copy.start()

    def arrived(ref, sem):
        pltpu.make_async_remote_copy(
            src_ref=ref, dst_ref=ref, send_sem=sem, recv_sem=sem, device_id=partner, device_id_type=MESH
        ).wait_recv()

    def departed(ref, sem):
        pltpu.make_async_remote_copy(
            src_ref=ref, dst_ref=ref, send_sem=sem, recv_sem=sem, device_id=partner, device_id_type=MESH
        ).wait_send()

    def products(q, second):
        tokens = xs[q]
        for block in (a2, ap, am, a):
            if second:
                pair = ws[pl.ds(PIECES + 2 * block, 2)].reshape(2 * WIDTH, FEATURES)
                term = lax.dot_general(tokens, pair, (((1,), (1,)), ((), ())), preferred_element_type=F32)
            else:
                pair = jnp.concatenate([ws[2 * block], ws[2 * block + 1]], axis=1)
                term = jnp.dot(tokens, pair, preferred_element_type=F32)
            for h in range(2):
                half = term[:, h * WIDTH : (h + 1) * WIDTH]
                if block is a:
                    own[q, h] = half
                else:
                    part[q, 2 * block + h] = half.astype(BF16)

    load_x = [
        pltpu.make_async_copy(pat_h.at[0], xs.at[0], ld.at[0]),
        pltpu.make_async_copy(cot_h.at[0], xs.at[BLOCKS], ld.at[1]),
    ]
    load_win = [
        pltpu.make_async_copy(win_h.at[:, pl.ds(p * WIDTH, WIDTH)], ws.at[p], ld.at[4 + p]) for p in range(PIECES)
    ]
    load_wout = pltpu.make_async_copy(wout_h, ws.at[pl.ds(PIECES, PIECES)], ld.at[2])
    load_mout = pltpu.make_async_copy(mout_h, mom.at[pl.ds(PIECES, PIECES)], ld.at[3])
    load_min = [
        pltpu.make_async_copy(min_h.at[0, :, pl.ds(p * WIDTH, WIDTH)], mom.at[p], ld.at[4 + PIECES + p])
        for p in range(PIECES)
    ]
    for copy in load_x + load_win + [load_wout]:
        copy.start()

    barrier = pltpu.get_barrier_semaphore()
    peers = [to_ap, to_am, to_bp, to_bm, partner] + [(row, (col + d) % BLOCKS, rep) for d in range(1, BLOCKS)]
    for device in peers:
        pl.semaphore_signal(barrier, inc=1, device_id=device, device_id_type=MESH)
    for copy in load_x + load_win:
        copy.wait()
    products(0, False)
    pl.semaphore_wait(barrier, len(peers))

    for base in (0, BLOCKS):
        for slot in range(1, BLOCKS):
            target = (row, (col - token_offset(slot) + BLOCKS) % BLOCKS, rep)
            send(xs.at[base], xs.at[base + slot], zsend.at[base + slot], zrecv.at[base + slot], target)

    load_wout.wait()
    for copy in load_min + [load_mout]:
        copy.start()

    def prepare(q):
        @pl.when(q % BLOCKS != 0)
        def _():
            arrived(xs.at[q], zrecv.at[q])

        @pl.when(q < BLOCKS)
        def _():
            products(q, False)

        @pl.when(q >= BLOCKS)
        def _():
            products(q, True)

    def reduce_start(q):
        send(part.at[q, 2 * a2], t1.at[q, 0], rsend.at[0, q], rrecv.at[0, q], to_ap)
        send(part.at[q, 2 * a2 + 1], t1.at[q, 1], rsend.at[0, q], rrecv.at[0, q], to_am)
        send(part.at[q, 2 * ap + 1], r1.at[q, 1], rsend.at[0, q], rrecv.at[1, q], to_ap)
        send(part.at[q, 2 * am], r1.at[q, 2], rsend.at[0, q], rrecv.at[1, q], to_am)

    def reduce_relay(q):
        arrived(t1.at[q], rrecv.at[0, q])
        part[q, 2 * ap] = (part[q, 2 * ap].astype(F32) + t1[q, 0].astype(F32)).astype(BF16)
        part[q, 2 * am + 1] = (part[q, 2 * am + 1].astype(F32) + t1[q, 1].astype(F32)).astype(BF16)
        send(part.at[q, 2 * ap], r1.at[q, 0], rsend.at[1, q], rrecv.at[1, q], to_ap)
        send(part.at[q, 2 * am + 1], r1.at[q, 3], rsend.at[1, q], rrecv.at[1, q], to_am)

    def second_start(q):
        arrived(r1.at[q], rrecv.at[1, q])
        for h in range(2):
            total = own[q, h] + r1[q, h].astype(F32) + r1[q, 2 + h].astype(F32)
            total = total.reshape(RING, SUB, WIDTH)
            total_s[q, h] = total
            summed[q, h] = total.astype(BF16)
        send(summed.at[q, 0, b2], t2.at[q, 0], rsend.at[2, q], rrecv.at[2, q], to_bp)
        send(summed.at[q, 1, b2], t2.at[q, 1], rsend.at[2, q], rrecv.at[2, q], to_bm)
        send(summed.at[q, 1, bp], r2.at[q, 1], rsend.at[2, q], rrecv.at[3, q], to_bp)
        send(summed.at[q, 0, bm], r2.at[q, 2], rsend.at[2, q], rrecv.at[3, q], to_bm)

    def second_relay(q):
        arrived(t2.at[q], rrecv.at[2, q])
        summed[q, 0, bp] = (summed[q, 0, bp].astype(F32) + t2[q, 0].astype(F32)).astype(BF16)
        summed[q, 1, bm] = (summed[q, 1, bm].astype(F32) + t2[q, 1].astype(F32)).astype(BF16)
        send(summed.at[q, 0, bp], r2.at[q, 0], rsend.at[3, q], rrecv.at[3, q], to_bp)
        send(summed.at[q, 1, bm], r2.at[q, 3], rsend.at[3, q], rrecv.at[3, q], to_bm)

    def activate(q):
        arrived(r2.at[q], rrecv.at[3, q])
        totals = [
            total_s[q, h, b] + r2[q, h].astype(F32) + r2[q, 2 + h].astype(F32) for h in range(2)
        ]

        @pl.when(q < BLOCKS)
        def _():
            for h in range(2):
                pre_s[q, h] = totals[h]
                act[q, 2 * a + h, b] = gelu_value(totals[h]).astype(BF16)

        @pl.when(q >= BLOCKS)
        def _():
            for h in range(2):
                slope = gelu_slope(pre_s[q - BLOCKS, h])
                act[q, 2 * a + h, b] = (totals[h] * slope).astype(BF16)

        mine = act.at[q, pl.ds(2 * a, 2), b]
        send(mine, mine, asend.at[0, q], arecv.at[0, q], to_bp)
        send(mine, mine, asend.at[0, q], arecv.at[0, q], to_bm)

    def second_spread(q):
        arrived(part.at[q, 0], arecv.at[0, q])
        ahead, behind = act.at[q, 2 * a, bm], act.at[q, 2 * a + 1, bp]
        send(ahead, ahead, asend.at[1, q], arecv.at[1, q], to_bp)
        send(behind, behind, asend.at[1, q], arecv.at[1, q], to_bm)

    def first_spread(q):
        arrived(t2.at[q], arecv.at[1, q])
        near, far = act.at[q, 2 * a], act.at[q, 2 * a + 1]
        send(near, near, asend.at[2, q], arecv.at[2, q], to_ap)
        send(far, far, asend.at[2, q], arecv.at[2, q], to_am)
        send(far, far, asend.at[2, q], arecv.at[4, q], to_ap)
        send(near, near, asend.at[2, q], arecv.at[4, q], to_am)

    def first_relay(q):
        arrived(t1.at[q], arecv.at[2, q])
        ahead, behind = act.at[q, 2 * am], act.at[q, 2 * ap + 1]
        send(ahead, ahead, asend.at[3, q], arecv.at[3, q], to_ap)
        send(behind, behind, asend.at[3, q], arecv.at[3, q], to_am)

    def complete(q):
        arrived(t1.at[q], arecv.at[4, q])
        arrived(t1.at[q], arecv.at[3, q])

        @pl.when(q < BLOCKS)
        def _():
            total = jnp.zeros((TOKENS, FEATURES), F32)
            for p in range(PIECES):
                total += jnp.dot(
                    act[q, p].reshape(TOKENS, WIDTH), ws[PIECES + p], preferred_element_type=F32
                )

            mpart[q] = total

            @pl.when(q % 2 == 1)
            def _():
                rows = pl.ds(pl.multiple_of((q - 1) * TOKENS, 2 * TOKENS), 2 * TOKENS)
                for p in range(PIECES):
                    hid_t[p, :, rows] = act[pl.ds(q - 1, 2), p].reshape(2 * TOKENS, WIDTH).T

            @pl.when(q > 0)
            def _():
                target = (row, (col + token_offset(q) + BLOCKS) % BLOCKS, rep)
                send(mpart.at[q], mrecv.at[q], msend.at[q], mrcv.at[q], target)

    grad_factor = (1.0 - momentum_decay) / vote_scale / math.sqrt(BLOCKS * TOKENS)
    moment_factor = momentum_decay / vote_scale

    def vote(grad, index):
        moved = moment_factor * mom[index].astype(F32) + grad_factor * grad
        votes[index] = jnp.tanh(moved).astype(BF16)
        send(votes.at[index], tallies.at[index], vsend.at[index], vrcv.at[index], partner)

    def vote_second(p):
        cotangent = xs[pl.ds(BLOCKS, BLOCKS)].reshape(BLOCKS * TOKENS, FEATURES)
        grad = jnp.dot(hid_t[p], cotangent, preferred_element_type=F32)
        vote(grad, PIECES + p)

    def vote_first(block):
        pieces = [act[pl.ds(BLOCKS, BLOCKS), 2 * block + h].reshape(BLOCKS * TOKENS, WIDTH) for h in range(2)]
        grad = jnp.dot(pat_t[...], jnp.concatenate(pieces, axis=1), preferred_element_type=F32)
        for h in range(2):
            vote(grad[:, h * WIDTH : (h + 1) * WIDTH], 2 * block + h)

    def tally(index):
        arrived(tallies.at[index], vrcv.at[index])
        tallies[index] = votes[index] + tallies[index]

    stages = (
        reduce_start, reduce_relay, second_start, second_relay, activate,
        second_spread, first_spread, first_relay, complete,
    )

    def turn(i, carry):
        for lag, stage in zip(LAGS, stages):

            @pl.when((i >= lag) & (i < UNITS + lag))
            def _(lag=lag, stage=stage):
                stage(unit_at(i - lag))

        @pl.when(i < UNITS - 1)
        def _():
            prepare(unit_at(i + 1))

        @pl.when(i == TURNS - BLOCKS)
        def _():
            load_mout.wait()
            pat_t[...] = xs[pl.ds(0, BLOCKS)].reshape(BLOCKS * TOKENS, FEATURES).T

        @pl.when(i >= TURNS - BLOCKS)
        def _():
            vote_second(i - (TURNS - BLOCKS))

        @pl.when(i >= TURNS - TALLY_TURNS)
        def _():
            tally(PIECES + i - (TURNS - TALLY_TURNS))

        return carry

    lax.fori_loop(0, TURNS, turn, 0)

    for copy in load_min:
        copy.wait()

    def first_turn(p, carry):
        vote_first(p)
        return carry

    lax.fori_loop(0, PIECES // 2, first_turn, 0)

    def second_tally(p, carry):
        tally(PIECES + p)
        return carry

    lax.fori_loop(TALLY_TURNS, PIECES, second_tally, 0)

    total = mpart[0]
    for slot in range(1, BLOCKS):
        arrived(mrecv.at[slot], mrcv.at[slot])
        total += mrecv[slot]
    mixed_v[...] = total.astype(BF16)

    def first_tally(p, carry):
        tally(p)
        return carry

    lax.fori_loop(0, PIECES, first_tally, 0)

    def drain(q, carry):
        departed(part.at[q, pl.ds(0, 4)], rsend.at[0, q])
        departed(part.at[q, pl.ds(0, 2)], rsend.at[1, q])
        departed(summed.at[q, 0], rsend.at[2, q])
        departed(t2.at[q], rsend.at[3, q])
        departed(summed.at[q, 0], asend.at[0, q])
        departed(t2.at[q], asend.at[1, q])
        departed(part.at[q, pl.ds(0, 4)], asend.at[2, q])
        departed(part.at[q, pl.ds(0, 2)], asend.at[3, q])
        departed(votes.at[q], vsend.at[q])

        @pl.when(q % BLOCKS != 0)
        def _():
            departed(xs.at[q], zsend.at[q])

        return carry

    lax.fori_loop(0, UNITS, drain, 0)
    for slot in range(1, BLOCKS):
        departed(mpart.at[slot], msend.at[slot])


def output_kernel(mixed_v, tallies, mixed_o, tin_o, tout_o, sems):
    copies = [
        pltpu.make_async_copy(mixed_v, mixed_o.at[0], sems.at[0]),
        pltpu.make_async_copy(tallies.at[pl.ds(PIECES, PIECES)], tout_o, sems.at[1]),
    ]
    for p in range(PIECES):
        columns = tin_o.at[:, pl.ds(p * WIDTH, WIDTH)]
        copies.append(pltpu.make_async_copy(tallies.at[p], columns, sems.at[2 + p]))
    for copy in copies:
        copy.start()
    for copy in copies:
        copy.wait()


def shards(patches, cotangent, w_in, w_out, moment_in, moment_out):
    by_piece = (PIECES, WIDTH, FEATURES)
    anywhere = pl.BlockSpec(memory_space=pl.ANY)
    in_vmem = pl.BlockSpec(memory_space=pltpu.VMEM)
    results = pl.pallas_call(
        step_kernel,
        out_shape=(
            pltpu.VMEM((TOKENS, FEATURES), BF16),
            pltpu.VMEM((UNITS, WIDTH, FEATURES), BF16),
        ),
        in_specs=[anywhere] * 6,
        out_specs=(in_vmem,) * 2,
        scratch_shapes=[
            pltpu.VMEM((UNITS, TOKENS, FEATURES), BF16),
            pltpu.VMEM((UNITS, WIDTH, FEATURES), BF16),
            pltpu.VMEM((UNITS, WIDTH, FEATURES), BF16),
            pltpu.VMEM((UNITS, PIECES, TOKENS, WIDTH), BF16),
            pltpu.VMEM((UNITS, 2, TOKENS, WIDTH), F32),
            pltpu.VMEM((UNITS, 2, TOKENS, WIDTH), BF16),
            pltpu.VMEM((UNITS, 4, TOKENS, WIDTH), BF16),
            pltpu.VMEM((UNITS, 2, RING, SUB, WIDTH), BF16),
            pltpu.VMEM((UNITS, 2, RING, SUB, WIDTH), F32),
            pltpu.VMEM((UNITS, 2, SUB, WIDTH), BF16),
            pltpu.VMEM((UNITS, 4, SUB, WIDTH), BF16),
            pltpu.VMEM((BLOCKS, 2, SUB, WIDTH), F32),
            pltpu.VMEM((UNITS, PIECES, RING, SUB, WIDTH), BF16),
            pltpu.VMEM((FEATURES, BLOCKS * TOKENS), BF16),
            pltpu.VMEM((PIECES, WIDTH, BLOCKS * TOKENS), BF16),
            pltpu.VMEM((BLOCKS, TOKENS, FEATURES), F32),
            pltpu.VMEM((BLOCKS, TOKENS, FEATURES), F32),
            pltpu.VMEM((UNITS, WIDTH, FEATURES), BF16),
            pltpu.SemaphoreType.DMA((4 + 2 * PIECES,)),
            pltpu.SemaphoreType.DMA((UNITS,)),
            pltpu.SemaphoreType.DMA((UNITS,)),
            pltpu.SemaphoreType.DMA((4, UNITS)),
            pltpu.SemaphoreType.DMA((4, UNITS)),
            pltpu.SemaphoreType.DMA((4, UNITS)),
            pltpu.SemaphoreType.DMA((5, UNITS)),
            pltpu.SemaphoreType.DMA((BLOCKS,)),
            pltpu.SemaphoreType.DMA((BLOCKS,)),
            pltpu.SemaphoreType.DMA((UNITS,)),
            pltpu.SemaphoreType.DMA((UNITS,)),
        ],
        compiler_params=pltpu.CompilerParams(
            collective_id=0, has_side_effects=True, vmem_limit_bytes=VMEM_LIMIT
        ),
    )(
        patches, cotangent, w_in, w_out.reshape(by_piece), moment_in, moment_out[0].reshape(by_piece),
    )
    mixed, tally_first, tally_second = pl.pallas_call(
        output_kernel,
        out_shape=(
            jax.ShapeDtypeStruct((1, TOKENS, FEATURES), BF16),
            jax.ShapeDtypeStruct((FEATURES, PIECES * WIDTH), BF16),
            jax.ShapeDtypeStruct(by_piece, BF16),
        ),
        in_specs=[in_vmem] * 2,
        out_specs=(anywhere,) * 3,
        scratch_shapes=[pltpu.SemaphoreType.DMA((2 + PIECES,))],
        compiler_params=pltpu.CompilerParams(vmem_limit_bytes=2**20),
    )(*results)
    return mixed, tally_first, tally_second.reshape(PIECES * WIDTH, FEATURES)


def solution(mesh):
    in_specs = (
        P("rep", "col", "row"),
        P("rep", "col", "row"),
        P("row", "col"),
        P("col", "row"),
        P("rep", "row", "col"),
        P("rep", "col", "row"),
    )
    out_specs = (P("rep", "col", "row"), P("row", "col"), P("col", "row"))
    return jax.shard_map(shards, mesh=mesh, in_specs=in_specs, out_specs=out_specs, check_vma=False)
```

```python
import math

import jax
import jax.numpy as jnp
from jax import lax
from jax.experimental import pallas as pl
from jax.experimental.pallas import tpu as pltpu
from jax.sharding import PartitionSpec as P

MESH = pl.DeviceIdType.MESH
BF16, F32 = jnp.bfloat16, jnp.float32

momentum_decay = 0.9
vote_scale = 0.3

BLOCKS, TOKENS, FEATURES, PIECES, WIDTH = 8, 64, 384, 8, 384
UNITS = 2 * BLOCKS
RING = 4
SUB = TOKENS // RING
LAGS = (0, 2, 5, 7, 10, 12, 15, 19, 23)
VMEM_LIMIT = 50 * 1024 * 1024
TURNS = UNITS + LAGS[-1]


def gelu_value(pre):
    return 0.5 * pre * (1.0 + lax.erf(pre * (1.0 / math.sqrt(2.0))))


def gelu_slope(pre):
    return 0.5 * (1.0 + lax.erf(pre * (1.0 / math.sqrt(2.0)))) + pre * jnp.exp(-0.5 * pre * pre) * (
        1.0 / math.sqrt(2.0 * math.pi)
    )


def unit_at(place):
    moved = jnp.where(place <= BLOCKS, place - 1, place)
    return jnp.where(place == 0, 0, jnp.where(place == 1, BLOCKS, moved))


def token_offset(slot):
    return ((slot + 1) // 2) * ((slot % 2) * 2 - 1)


def step_kernel(
    pat_h, cot_h, win_h, wout_h, min_h, mout_h,
    mixed_v, votes, theirs,
    xs, ws, mom, part, own, t1, r1, summed, total_s, t2, r2, pre_s, act, pat_t, hid_t,
    mpart, mrecv,
    ld, zsend, zrecv, rsend, rrecv, asend, arecv, msend, mrcv, vsend, vrcv,
):
    row, col, rep = lax.axis_index("row"), lax.axis_index("col"), lax.axis_index("rep")
    x, y = row % RING, row // RING
    a = x * (1 - rep) + y * rep
    b = y * (1 - rep) + x * rep

    def peer(a_to, b_to):
        x_to = a_to * (1 - rep) + b_to * rep
        y_to = b_to * (1 - rep) + a_to * rep
        return (y_to * RING + x_to, col, rep)

    ap, am, a2 = (a + 1) % RING, (a + 3) % RING, (a + 2) % RING
    bp, bm, b2 = (b + 1) % RING, (b + 3) % RING, (b + 2) % RING
    to_ap, to_am, to_bp, to_bm = peer(ap, b), peer(am, b), peer(a, bp), peer(a, bm)
    partner = (row, col, 1 - rep)

    def send(src, dst, send_sem, recv_sem, device):
        copy = pltpu.make_async_remote_copy(
            src_ref=src, dst_ref=dst, send_sem=send_sem, recv_sem=recv_sem,
            device_id=device, device_id_type=MESH,
        )
        copy.start()

    def arrived(ref, sem):
        pltpu.make_async_remote_copy(
            src_ref=ref, dst_ref=ref, send_sem=sem, recv_sem=sem, device_id=partner, device_id_type=MESH
        ).wait_recv()

    def departed(ref, sem):
        pltpu.make_async_remote_copy(
            src_ref=ref, dst_ref=ref, send_sem=sem, recv_sem=sem, device_id=partner, device_id_type=MESH
        ).wait_send()

    def products(q, second):
        tokens = xs[q]
        for block in (a2, ap, am, a):
            if second:
                pair = ws[pl.ds(PIECES + 2 * block, 2)].reshape(2 * WIDTH, FEATURES)
                term = lax.dot_general(tokens, pair, (((1,), (1,)), ((), ())), preferred_element_type=F32)
            else:
                pair = jnp.concatenate([ws[2 * block], ws[2 * block + 1]], axis=1)
                term = jnp.dot(tokens, pair, preferred_element_type=F32)
            for h in range(2):
                half = term[:, h * WIDTH : (h + 1) * WIDTH]
                if block is a:
                    own[q, h] = half
                else:
                    part[q, 2 * block + h] = half.astype(BF16)

    load_x = [
        pltpu.make_async_copy(pat_h.at[0], xs.at[0], ld.at[0]),
        pltpu.make_async_copy(cot_h.at[0], xs.at[BLOCKS], ld.at[1]),
    ]
    load_win = [
        pltpu.make_async_copy(win_h.at[:, pl.ds(p * WIDTH, WIDTH)], ws.at[p], ld.at[4 + p]) for p in range(PIECES)
    ]
    load_wout = pltpu.make_async_copy(wout_h, ws.at[pl.ds(PIECES, PIECES)], ld.at[2])
    load_mout = pltpu.make_async_copy(mout_h, mom.at[pl.ds(PIECES, PIECES)], ld.at[3])
    load_min = [
        pltpu.make_async_copy(min_h.at[0, :, pl.ds(p * WIDTH, WIDTH)], mom.at[p], ld.at[4 + PIECES + p])
        for p in range(PIECES)
    ]
    for copy in load_x + load_win + [load_wout]:
        copy.start()

    barrier = pltpu.get_barrier_semaphore()
    below, above = (row, (col + BLOCKS - 1) % BLOCKS, rep), (row, (col + 1) % BLOCKS, rep)
    peers = [to_ap, to_am, to_bp, to_bm, partner, below, above]
    for device in peers:
        pl.semaphore_signal(barrier, inc=1, device_id=device, device_id_type=MESH)
    for copy in load_x + load_win:
        copy.wait()
    products(0, False)
    pl.semaphore_wait(barrier, len(peers))

    for base in (0, BLOCKS):
        send(xs.at[base], xs.at[base + 1], zsend.at[base + 1], zrecv.at[base + 1], below)
        send(xs.at[base], xs.at[base + 2], zsend.at[base + 2], zrecv.at[base + 2], above)

    load_wout.wait()
    for copy in load_min + [load_mout]:
        copy.start()

    def prepare(q):
        @pl.when(q % BLOCKS != 0)
        def _():
            arrived(xs.at[q], zrecv.at[q])

        @pl.when((q % BLOCKS >= 1) & (q % BLOCKS < BLOCKS - 2))
        def _():
            onward = (row, (col + BLOCKS + 1 - 2 * (q % 2)) % BLOCKS, rep)
            send(xs.at[q], xs.at[q + 2], zsend.at[q + 2], zrecv.at[q + 2], onward)

        @pl.when(q < BLOCKS)
        def _():
            products(q, False)

        @pl.when(q >= BLOCKS)
        def _():
            products(q, True)

    def reduce_start(q):
        send(part.at[q, 2 * a2], t1.at[q, 0], rsend.at[0, q], rrecv.at[0, q], to_ap)
        send(part.at[q, 2 * a2 + 1], t1.at[q, 1], rsend.at[0, q], rrecv.at[0, q], to_am)
        send(part.at[q, 2 * ap + 1], r1.at[q, 1], rsend.at[0, q], rrecv.at[1, q], to_ap)
        send(part.at[q, 2 * am], r1.at[q, 2], rsend.at[0, q], rrecv.at[1, q], to_am)

    def reduce_relay(q):
        arrived(t1.at[q], rrecv.at[0, q])
        part[q, 2 * ap] = (part[q, 2 * ap].astype(F32) + t1[q, 0].astype(F32)).astype(BF16)
        part[q, 2 * am + 1] = (part[q, 2 * am + 1].astype(F32) + t1[q, 1].astype(F32)).astype(BF16)
        send(part.at[q, 2 * ap], r1.at[q, 0], rsend.at[1, q], rrecv.at[1, q], to_ap)
        send(part.at[q, 2 * am + 1], r1.at[q, 3], rsend.at[1, q], rrecv.at[1, q], to_am)

    def second_start(q):
        arrived(r1.at[q], rrecv.at[1, q])
        for h in range(2):
            total = own[q, h] + r1[q, h].astype(F32) + r1[q, 2 + h].astype(F32)
            total = total.reshape(RING, SUB, WIDTH)
            total_s[q, h] = total
            summed[q, h] = total.astype(BF16)
        send(summed.at[q, 0, b2], t2.at[q, 0], rsend.at[2, q], rrecv.at[2, q], to_bp)
        send(summed.at[q, 1, b2], t2.at[q, 1], rsend.at[2, q], rrecv.at[2, q], to_bm)
        send(summed.at[q, 1, bp], r2.at[q, 1], rsend.at[2, q], rrecv.at[3, q], to_bp)
        send(summed.at[q, 0, bm], r2.at[q, 2], rsend.at[2, q], rrecv.at[3, q], to_bm)

    def second_relay(q):
        arrived(t2.at[q], rrecv.at[2, q])
        summed[q, 0, bp] = (summed[q, 0, bp].astype(F32) + t2[q, 0].astype(F32)).astype(BF16)
        summed[q, 1, bm] = (summed[q, 1, bm].astype(F32) + t2[q, 1].astype(F32)).astype(BF16)
        send(summed.at[q, 0, bp], r2.at[q, 0], rsend.at[3, q], rrecv.at[3, q], to_bp)
        send(summed.at[q, 1, bm], r2.at[q, 3], rsend.at[3, q], rrecv.at[3, q], to_bm)

    def activate(q):
        arrived(r2.at[q], rrecv.at[3, q])
        totals = [
            total_s[q, h, b] + r2[q, h].astype(F32) + r2[q, 2 + h].astype(F32) for h in range(2)
        ]

        @pl.when(q < BLOCKS)
        def _():
            for h in range(2):
                pre_s[q, h] = totals[h]
                act[q, 2 * a + h, b] = gelu_value(totals[h]).astype(BF16)

        @pl.when(q >= BLOCKS)
        def _():
            for h in range(2):
                slope = gelu_slope(pre_s[q - BLOCKS, h])
                act[q, 2 * a + h, b] = (totals[h] * slope).astype(BF16)

        mine = act.at[q, pl.ds(2 * a, 2), b]
        send(mine, mine, asend.at[0, q], arecv.at[0, q], to_bp)
        send(mine, mine, asend.at[0, q], arecv.at[0, q], to_bm)

    def second_spread(q):
        arrived(part.at[q, 0], arecv.at[0, q])
        ahead, behind = act.at[q, 2 * a, bm], act.at[q, 2 * a + 1, bp]
        send(ahead, ahead, asend.at[1, q], arecv.at[1, q], to_bp)
        send(behind, behind, asend.at[1, q], arecv.at[1, q], to_bm)

    def first_spread(q):
        arrived(t2.at[q], arecv.at[1, q])
        near, far = act.at[q, 2 * a], act.at[q, 2 * a + 1]
        send(near, near, asend.at[2, q], arecv.at[2, q], to_ap)
        send(far, far, asend.at[2, q], arecv.at[2, q], to_am)
        send(far, far, asend.at[2, q], arecv.at[4, q], to_ap)
        send(near, near, asend.at[2, q], arecv.at[4, q], to_am)

    def first_relay(q):
        arrived(t1.at[q], arecv.at[2, q])
        ahead, behind = act.at[q, 2 * am], act.at[q, 2 * ap + 1]
        send(ahead, ahead, asend.at[3, q], arecv.at[3, q], to_ap)
        send(behind, behind, asend.at[3, q], arecv.at[3, q], to_am)

    def complete(q):
        arrived(t1.at[q], arecv.at[4, q])
        arrived(t1.at[q], arecv.at[3, q])

        @pl.when(q < BLOCKS)
        def _():
            total = jnp.zeros((TOKENS, FEATURES), F32)
            for p in range(PIECES):
                total += jnp.dot(
                    act[q, p].reshape(TOKENS, WIDTH), ws[PIECES + p], preferred_element_type=F32
                )

            mpart[q] = total

            @pl.when(q % 2 == 1)
            def _():
                rows = pl.ds(pl.multiple_of((q - 1) * TOKENS, 2 * TOKENS), 2 * TOKENS)
                for p in range(PIECES):
                    hid_t[p, :, rows] = act[pl.ds(q - 1, 2), p].reshape(2 * TOKENS, WIDTH).T

            @pl.when(q > 0)
            def _():
                target = (row, (col + token_offset(q) + BLOCKS) % BLOCKS, rep)
                send(mpart.at[q], mrecv.at[q], msend.at[q], mrcv.at[q], target)

    grad_factor = (1.0 - momentum_decay) / vote_scale / math.sqrt(BLOCKS * TOKENS)
    moment_factor = momentum_decay / vote_scale

    def vote(grad, index):
        moved = moment_factor * mom[index].astype(F32) + grad_factor * grad
        votes[index] = jnp.tanh(moved).astype(BF16)
        send(votes.at[index], theirs.at[index], vsend.at[index], vrcv.at[index], partner)

    def vote_second(p):
        cotangent = xs[pl.ds(BLOCKS, BLOCKS)].reshape(BLOCKS * TOKENS, FEATURES)
        grad = jnp.dot(hid_t[p], cotangent, preferred_element_type=F32)
        vote(grad, PIECES + p)

    def vote_first(block):
        pieces = [act[pl.ds(BLOCKS, BLOCKS), 2 * block + h].reshape(BLOCKS * TOKENS, WIDTH) for h in range(2)]
        grad = jnp.dot(pat_t[...], jnp.concatenate(pieces, axis=1), preferred_element_type=F32)
        for h in range(2):
            vote(grad[:, h * WIDTH : (h + 1) * WIDTH], 2 * block + h)

    stages = (
        reduce_start, reduce_relay, second_start, second_relay, activate,
        second_spread, first_spread, first_relay, complete,
    )

    def turn(i, carry):
        for lag, stage in zip(LAGS, stages):

            @pl.when((i >= lag) & (i < UNITS + lag))
            def _(lag=lag, stage=stage):
                stage(unit_at(i - lag))

        @pl.when(i < UNITS - 1)
        def _():
            prepare(unit_at(i + 1))

        @pl.when(i == TURNS - BLOCKS)
        def _():
            load_mout.wait()
            pat_t[...] = xs[pl.ds(0, BLOCKS)].reshape(BLOCKS * TOKENS, FEATURES).T

        @pl.when(i >= TURNS - BLOCKS)
        def _():
            vote_second(i - (TURNS - BLOCKS))

        return carry

    lax.fori_loop(0, TURNS, turn, 0)

    for copy in load_min:
        copy.wait()

    def first_turn(p, carry):
        vote_first(p)
        return carry

    lax.fori_loop(0, PIECES // 2, first_turn, 0)

    total = mpart[0]
    for slot in range(1, BLOCKS):
        arrived(mrecv.at[slot], mrcv.at[slot])
        total += mrecv[slot]
    mixed_v[...] = total.astype(BF16)

    def drain(q, carry):
        departed(part.at[q, pl.ds(0, 4)], rsend.at[0, q])
        departed(part.at[q, pl.ds(0, 2)], rsend.at[1, q])
        departed(summed.at[q, 0], rsend.at[2, q])
        departed(t2.at[q], rsend.at[3, q])
        departed(summed.at[q, 0], asend.at[0, q])
        departed(t2.at[q], asend.at[1, q])
        departed(part.at[q, pl.ds(0, 4)], asend.at[2, q])
        departed(part.at[q, pl.ds(0, 2)], asend.at[3, q])
        departed(votes.at[q], vsend.at[q])
        arrived(theirs.at[q], vrcv.at[q])

        @pl.when(q % BLOCKS != 0)
        def _():
            departed(xs.at[q], zsend.at[q])

        return carry

    lax.fori_loop(0, UNITS, drain, 0)
    for slot in range(1, BLOCKS):
        departed(mpart.at[slot], msend.at[slot])


def output_kernel(mixed_v, votes, theirs, mixed_o, tin_o, tout_o, tallies, sems):
    copies = [pltpu.make_async_copy(mixed_v, mixed_o.at[0], sems.at[UNITS])]
    copies[0].start()
    for index in [*range(PIECES, UNITS), *range(PIECES)]:
        tallies[index] = votes[index] + theirs[index]
        if index < PIECES:
            target = tin_o.at[:, pl.ds(index * WIDTH, WIDTH)]
        else:
            target = tout_o.at[index - PIECES]
        copies.append(pltpu.make_async_copy(tallies.at[index], target, sems.at[index]))
        copies[-1].start()
    for copy in copies:
        copy.wait()


def shards(patches, cotangent, w_in, w_out, moment_in, moment_out):
    by_piece = (PIECES, WIDTH, FEATURES)
    anywhere = pl.BlockSpec(memory_space=pl.ANY)
    in_vmem = pl.BlockSpec(memory_space=pltpu.VMEM)
    results = pl.pallas_call(
        step_kernel,
        out_shape=(
            pltpu.VMEM((TOKENS, FEATURES), BF16),
            pltpu.VMEM((UNITS, WIDTH, FEATURES), BF16),
            pltpu.VMEM((UNITS, WIDTH, FEATURES), BF16),
        ),
        in_specs=[anywhere] * 6,
        out_specs=(in_vmem,) * 3,
        scratch_shapes=[
            pltpu.VMEM((UNITS, TOKENS, FEATURES), BF16),
            pltpu.VMEM((UNITS, WIDTH, FEATURES), BF16),
            pltpu.VMEM((UNITS, WIDTH, FEATURES), BF16),
            pltpu.VMEM((UNITS, PIECES, TOKENS, WIDTH), BF16),
            pltpu.VMEM((UNITS, 2, TOKENS, WIDTH), F32),
            pltpu.VMEM((UNITS, 2, TOKENS, WIDTH), BF16),
            pltpu.VMEM((UNITS, 4, TOKENS, WIDTH), BF16),
            pltpu.VMEM((UNITS, 2, RING, SUB, WIDTH), BF16),
            pltpu.VMEM((UNITS, 2, RING, SUB, WIDTH), F32),
            pltpu.VMEM((UNITS, 2, SUB, WIDTH), BF16),
            pltpu.VMEM((UNITS, 4, SUB, WIDTH), BF16),
            pltpu.VMEM((BLOCKS, 2, SUB, WIDTH), F32),
            pltpu.VMEM((UNITS, PIECES, RING, SUB, WIDTH), BF16),
            pltpu.VMEM((FEATURES, BLOCKS * TOKENS), BF16),
            pltpu.VMEM((PIECES, WIDTH, BLOCKS * TOKENS), BF16),
            pltpu.VMEM((BLOCKS, TOKENS, FEATURES), F32),
            pltpu.VMEM((BLOCKS, TOKENS, FEATURES), F32),
            pltpu.SemaphoreType.DMA((4 + 2 * PIECES,)),
            pltpu.SemaphoreType.DMA((UNITS,)),
            pltpu.SemaphoreType.DMA((UNITS,)),
            pltpu.SemaphoreType.DMA((4, UNITS)),
            pltpu.SemaphoreType.DMA((4, UNITS)),
            pltpu.SemaphoreType.DMA((4, UNITS)),
            pltpu.SemaphoreType.DMA((5, UNITS)),
            pltpu.SemaphoreType.DMA((BLOCKS,)),
            pltpu.SemaphoreType.DMA((BLOCKS,)),
            pltpu.SemaphoreType.DMA((UNITS,)),
            pltpu.SemaphoreType.DMA((UNITS,)),
        ],
        compiler_params=pltpu.CompilerParams(
            collective_id=0, has_side_effects=True, vmem_limit_bytes=VMEM_LIMIT
        ),
    )(
        patches, cotangent, w_in, w_out.reshape(by_piece), moment_in, moment_out[0].reshape(by_piece),
    )
    mixed, tally_first, tally_second = pl.pallas_call(
        output_kernel,
        out_shape=(
            jax.ShapeDtypeStruct((1, TOKENS, FEATURES), BF16),
            jax.ShapeDtypeStruct((FEATURES, PIECES * WIDTH), BF16),
            jax.ShapeDtypeStruct(by_piece, BF16),
        ),
        in_specs=[in_vmem] * 3,
        out_specs=(anywhere,) * 3,
        scratch_shapes=[
            pltpu.VMEM((UNITS, WIDTH, FEATURES), BF16),
            pltpu.SemaphoreType.DMA((UNITS + 1,)),
        ],
        compiler_params=pltpu.CompilerParams(vmem_limit_bytes=8 * 2**20),
    )(*results)
    return mixed, tally_first, tally_second.reshape(PIECES * WIDTH, FEATURES)


def solution(mesh):
    in_specs = (
        P("rep", "col", "row"),
        P("rep", "col", "row"),
        P("row", "col"),
        P("col", "row"),
        P("rep", "row", "col"),
        P("rep", "col", "row"),
    )
    out_specs = (P("rep", "col", "row"), P("row", "col"), P("col", "row"))
    return jax.shard_map(shards, mesh=mesh, in_specs=in_specs, out_specs=out_specs, check_vma=False)
```

```python
import math

import jax
import jax.numpy as jnp
from jax import lax
from jax.experimental import pallas as pl
from jax.experimental.pallas import tpu as pltpu
from jax.sharding import PartitionSpec as P

MESH = pl.DeviceIdType.MESH
BF16, F32 = jnp.bfloat16, jnp.float32

momentum_decay = 0.9
vote_scale = 0.3

BLOCKS, TOKENS, FEATURES, PIECES, WIDTH = 8, 64, 384, 8, 384
UNITS = 2 * BLOCKS
RING = 4
SUB = TOKENS // RING
LAGS = (0, 2, 5, 7, 10, 13, 16, 21, 26)
VMEM_LIMIT = 50 * 1024 * 1024
TURNS = UNITS + LAGS[-1]


def gelu_value(pre):
    return 0.5 * pre * (1.0 + lax.erf(pre * (1.0 / math.sqrt(2.0))))


def gelu_slope(pre):
    return 0.5 * (1.0 + lax.erf(pre * (1.0 / math.sqrt(2.0)))) + pre * jnp.exp(-0.5 * pre * pre) * (
        1.0 / math.sqrt(2.0 * math.pi)
    )


def unit_at(place):
    moved = jnp.where(place <= BLOCKS, place - 1, place)
    return jnp.where(place == 0, 0, jnp.where(place == 1, BLOCKS, moved))


def token_offset(slot):
    return ((slot + 1) // 2) * ((slot % 2) * 2 - 1)


def step_kernel(
    pat_h, cot_h, win_h, wout_h, min_h, mout_h,
    mixed_v, votes, theirs,
    xs, ws, mom, part, own, t1, r1, summed, total_s, t2, r2, pre_s, act, pat_t, hid_t,
    mpart, mrecv,
    ld, zsend, zrecv, rsend, rrecv, asend, arecv, msend, mrcv, vsend, vrcv,
):
    row, col, rep = lax.axis_index("row"), lax.axis_index("col"), lax.axis_index("rep")
    x, y = row % RING, row // RING
    a = x * (1 - rep) + y * rep
    b = y * (1 - rep) + x * rep

    def peer(a_to, b_to):
        x_to = a_to * (1 - rep) + b_to * rep
        y_to = b_to * (1 - rep) + a_to * rep
        return (y_to * RING + x_to, col, rep)

    ap, am, a2 = (a + 1) % RING, (a + 3) % RING, (a + 2) % RING
    bp, bm, b2 = (b + 1) % RING, (b + 3) % RING, (b + 2) % RING
    to_ap, to_am, to_bp, to_bm = peer(ap, b), peer(am, b), peer(a, bp), peer(a, bm)
    partner = (row, col, 1 - rep)

    def send(src, dst, send_sem, recv_sem, device):
        copy = pltpu.make_async_remote_copy(
            src_ref=src, dst_ref=dst, send_sem=send_sem, recv_sem=recv_sem,
            device_id=device, device_id_type=MESH,
        )
        copy.start()

    def arrived(ref, sem):
        pltpu.make_async_remote_copy(
            src_ref=ref, dst_ref=ref, send_sem=sem, recv_sem=sem, device_id=partner, device_id_type=MESH
        ).wait_recv()

    def departed(ref, sem):
        pltpu.make_async_remote_copy(
            src_ref=ref, dst_ref=ref, send_sem=sem, recv_sem=sem, device_id=partner, device_id_type=MESH
        ).wait_send()

    def products(q, second):
        tokens = xs[q]
        for block in (a2, ap, am, a):
            if second:
                pair = ws[pl.ds(PIECES + 2 * block, 2)].reshape(2 * WIDTH, FEATURES)
                term = lax.dot_general(tokens, pair, (((1,), (1,)), ((), ())), preferred_element_type=F32)
            else:
                pair = jnp.concatenate([ws[2 * block], ws[2 * block + 1]], axis=1)
                term = jnp.dot(tokens, pair, preferred_element_type=F32)
            for h in range(2):
                half = term[:, h * WIDTH : (h + 1) * WIDTH]
                if block is a:
                    own[q, h] = half
                else:
                    part[q, 2 * block + h] = half.astype(BF16)

    load_x = [
        pltpu.make_async_copy(pat_h.at[0], xs.at[0], ld.at[0]),
        pltpu.make_async_copy(cot_h.at[0], xs.at[BLOCKS], ld.at[1]),
    ]
    load_win = [
        pltpu.make_async_copy(win_h.at[:, pl.ds(p * WIDTH, WIDTH)], ws.at[p], ld.at[4 + p]) for p in range(PIECES)
    ]
    load_wout = pltpu.make_async_copy(wout_h, ws.at[pl.ds(PIECES, PIECES)], ld.at[2])
    load_mout = pltpu.make_async_copy(mout_h, mom.at[pl.ds(PIECES, PIECES)], ld.at[3])
    load_min = [
        pltpu.make_async_copy(min_h.at[0, :, pl.ds(p * WIDTH, WIDTH)], mom.at[p], ld.at[4 + PIECES + p])
        for p in range(PIECES)
    ]
    barrier = pltpu.get_barrier_semaphore()
    below, above = (row, (col + BLOCKS - 1) % BLOCKS, rep), (row, (col + 1) % BLOCKS, rep)
    peers = [to_ap, to_am, to_bp, to_bm, partner, below, above]
    for device in peers:
        pl.semaphore_signal(barrier, inc=1, device_id=device, device_id_type=MESH)
    for copy in load_x + load_win + [load_wout]:
        copy.start()
    for copy in load_x + load_win:
        copy.wait()
    products(0, False)
    pl.semaphore_wait(barrier, len(peers))

    for base in (0, BLOCKS):
        send(xs.at[base], xs.at[base + 1], zsend.at[base + 1], zrecv.at[base + 1], below)
        send(xs.at[base], xs.at[base + 2], zsend.at[base + 2], zrecv.at[base + 2], above)

    load_wout.wait()
    for copy in load_min + [load_mout]:
        copy.start()

    def prepare(q):
        @pl.when(q % BLOCKS != 0)
        def _():
            arrived(xs.at[q], zrecv.at[q])

        @pl.when((q % BLOCKS >= 1) & (q % BLOCKS < BLOCKS - 2))
        def _():
            onward = (row, (col + BLOCKS + 1 - 2 * (q % 2)) % BLOCKS, rep)
            send(xs.at[q], xs.at[q + 2], zsend.at[q + 2], zrecv.at[q + 2], onward)

        @pl.when(q < BLOCKS)
        def _():
            products(q, False)

        @pl.when(q >= BLOCKS)
        def _():
            products(q, True)

    def reduce_start(q):
        send(part.at[q, 2 * a2], t1.at[q, 0], rsend.at[0, q], rrecv.at[0, q], to_ap)
        send(part.at[q, 2 * a2 + 1], t1.at[q, 1], rsend.at[0, q], rrecv.at[0, q], to_am)
        send(part.at[q, 2 * ap + 1], r1.at[q, 1], rsend.at[0, q], rrecv.at[1, q], to_ap)
        send(part.at[q, 2 * am], r1.at[q, 2], rsend.at[0, q], rrecv.at[1, q], to_am)

    def reduce_relay(q):
        arrived(t1.at[q], rrecv.at[0, q])
        part[q, 2 * ap] = (part[q, 2 * ap].astype(F32) + t1[q, 0].astype(F32)).astype(BF16)
        part[q, 2 * am + 1] = (part[q, 2 * am + 1].astype(F32) + t1[q, 1].astype(F32)).astype(BF16)
        send(part.at[q, 2 * ap], r1.at[q, 0], rsend.at[1, q], rrecv.at[1, q], to_ap)
        send(part.at[q, 2 * am + 1], r1.at[q, 3], rsend.at[1, q], rrecv.at[1, q], to_am)

    def second_start(q):
        arrived(r1.at[q], rrecv.at[1, q])
        for h in range(2):
            total = own[q, h] + r1[q, h].astype(F32) + r1[q, 2 + h].astype(F32)
            total = total.reshape(RING, SUB, WIDTH)
            total_s[q, h] = total
            summed[q, h] = total.astype(BF16)
        send(summed.at[q, 0, b2], t2.at[q, 0], rsend.at[2, q], rrecv.at[2, q], to_bp)
        send(summed.at[q, 1, b2], t2.at[q, 1], rsend.at[2, q], rrecv.at[2, q], to_bm)
        send(summed.at[q, 1, bp], r2.at[q, 1], rsend.at[2, q], rrecv.at[3, q], to_bp)
        send(summed.at[q, 0, bm], r2.at[q, 2], rsend.at[2, q], rrecv.at[3, q], to_bm)

    def second_relay(q):
        arrived(t2.at[q], rrecv.at[2, q])
        summed[q, 0, bp] = (summed[q, 0, bp].astype(F32) + t2[q, 0].astype(F32)).astype(BF16)
        summed[q, 1, bm] = (summed[q, 1, bm].astype(F32) + t2[q, 1].astype(F32)).astype(BF16)
        send(summed.at[q, 0, bp], r2.at[q, 0], rsend.at[3, q], rrecv.at[3, q], to_bp)
        send(summed.at[q, 1, bm], r2.at[q, 3], rsend.at[3, q], rrecv.at[3, q], to_bm)

    def activate(q):
        arrived(r2.at[q], rrecv.at[3, q])
        totals = [
            total_s[q, h, b] + r2[q, h].astype(F32) + r2[q, 2 + h].astype(F32) for h in range(2)
        ]

        @pl.when(q < BLOCKS)
        def _():
            for h in range(2):
                pre_s[q, h] = totals[h]
                act[q, 2 * a + h, b] = gelu_value(totals[h]).astype(BF16)

        @pl.when(q >= BLOCKS)
        def _():
            for h in range(2):
                slope = gelu_slope(pre_s[q - BLOCKS, h])
                act[q, 2 * a + h, b] = (totals[h] * slope).astype(BF16)

        mine = act.at[q, pl.ds(2 * a, 2), b]
        send(mine, mine, asend.at[0, q], arecv.at[0, q], to_bp)
        send(mine, mine, asend.at[0, q], arecv.at[0, q], to_bm)

    def second_spread(q):
        arrived(part.at[q, 0], arecv.at[0, q])
        ahead, behind = act.at[q, 2 * a, bm], act.at[q, 2 * a + 1, bp]
        send(ahead, ahead, asend.at[1, q], arecv.at[1, q], to_bp)
        send(behind, behind, asend.at[1, q], arecv.at[1, q], to_bm)

    def first_spread(q):
        arrived(t2.at[q], arecv.at[1, q])
        near, far = act.at[q, 2 * a], act.at[q, 2 * a + 1]
        send(near, near, asend.at[2, q], arecv.at[2, q], to_ap)
        send(far, far, asend.at[2, q], arecv.at[2, q], to_am)
        send(far, far, asend.at[2, q], arecv.at[4, q], to_ap)
        send(near, near, asend.at[2, q], arecv.at[4, q], to_am)

    def first_relay(q):
        arrived(t1.at[q], arecv.at[2, q])
        ahead, behind = act.at[q, 2 * am], act.at[q, 2 * ap + 1]
        send(ahead, ahead, asend.at[3, q], arecv.at[3, q], to_ap)
        send(behind, behind, asend.at[3, q], arecv.at[3, q], to_am)

    def complete(q):
        arrived(t1.at[q], arecv.at[4, q])
        arrived(t1.at[q], arecv.at[3, q])

        @pl.when(q < BLOCKS)
        def _():
            total = jnp.zeros((TOKENS, FEATURES), F32)
            for p in range(PIECES):
                total += jnp.dot(
                    act[q, p].reshape(TOKENS, WIDTH), ws[PIECES + p], preferred_element_type=F32
                )

            mpart[q] = total

            @pl.when(q % 2 == 1)
            def _():
                rows = pl.ds(pl.multiple_of((q - 1) * TOKENS, 2 * TOKENS), 2 * TOKENS)
                for p in range(PIECES):
                    hid_t[p, :, rows] = act[pl.ds(q - 1, 2), p].reshape(2 * TOKENS, WIDTH).T

            @pl.when(q > 0)
            def _():
                target = (row, (col + token_offset(q) + BLOCKS) % BLOCKS, rep)
                send(mpart.at[q], mrecv.at[q], msend.at[q], mrcv.at[q], target)

    grad_factor = (1.0 - momentum_decay) / vote_scale / math.sqrt(BLOCKS * TOKENS)
    moment_factor = momentum_decay / vote_scale

    def vote(grad, index):
        moved = moment_factor * mom[index].astype(F32) + grad_factor * grad
        votes[index] = jnp.tanh(moved).astype(BF16)
        send(votes.at[index], theirs.at[index], vsend.at[index], vrcv.at[index], partner)

    def vote_second(p):
        cotangent = xs[pl.ds(BLOCKS, BLOCKS)].reshape(BLOCKS * TOKENS, FEATURES)
        grad = jnp.dot(hid_t[p], cotangent, preferred_element_type=F32)
        vote(grad, PIECES + p)

    def vote_first(block):
        pieces = [act[pl.ds(BLOCKS, BLOCKS), 2 * block + h].reshape(BLOCKS * TOKENS, WIDTH) for h in range(2)]
        grad = jnp.dot(pat_t[...], jnp.concatenate(pieces, axis=1), preferred_element_type=F32)
        for h in range(2):
            vote(grad[:, h * WIDTH : (h + 1) * WIDTH], 2 * block + h)

    stages = (
        (LAGS[0], reduce_start), (LAGS[1], reduce_relay), (LAGS[7], first_relay), (LAGS[6], first_spread),
        (LAGS[2], second_start), (LAGS[3], second_relay), (LAGS[4], activate), (LAGS[5], second_spread),
        (LAGS[8], complete),
    )

    def turn(i, carry):
        for lag, stage in stages:

            @pl.when((i >= lag) & (i < UNITS + lag))
            def _(lag=lag, stage=stage):
                stage(unit_at(i - lag))

        @pl.when(i < UNITS - 1)
        def _():
            prepare(unit_at(i + 1))

        @pl.when(i == TURNS - BLOCKS)
        def _():
            load_mout.wait()
            pat_t[...] = xs[pl.ds(0, BLOCKS)].reshape(BLOCKS * TOKENS, FEATURES).T

        @pl.when(i >= TURNS - BLOCKS)
        def _():
            vote_second(i - (TURNS - BLOCKS))

        return carry

    lax.fori_loop(0, TURNS, turn, 0)

    for copy in load_min:
        copy.wait()

    def first_turn(p, carry):
        vote_first(p)
        return carry

    lax.fori_loop(0, PIECES // 2, first_turn, 0)

    total = mpart[0]
    for slot in range(1, BLOCKS):
        arrived(mrecv.at[slot], mrcv.at[slot])
        total += mrecv[slot]
    mixed_v[...] = total.astype(BF16)

    def drain(q, carry):
        departed(part.at[q, pl.ds(0, 4)], rsend.at[0, q])
        departed(part.at[q, pl.ds(0, 2)], rsend.at[1, q])
        departed(summed.at[q, 0], rsend.at[2, q])
        departed(t2.at[q], rsend.at[3, q])
        departed(summed.at[q, 0], asend.at[0, q])
        departed(t2.at[q], asend.at[1, q])
        departed(part.at[q, pl.ds(0, 4)], asend.at[2, q])
        departed(part.at[q, pl.ds(0, 2)], asend.at[3, q])
        departed(votes.at[q], vsend.at[q])

        @pl.when(q % BLOCKS != 0)
        def _():
            departed(xs.at[q], zsend.at[q])

        return carry

    lax.fori_loop(0, UNITS, drain, 0)
    for slot in range(1, BLOCKS):
        departed(mpart.at[slot], msend.at[slot])

    def theirs_in(q, carry):
        arrived(theirs.at[UNITS - 1 - q], vrcv.at[UNITS - 1 - q])
        return carry

    lax.fori_loop(0, UNITS, theirs_in, 0)


def output_kernel(mixed_v, votes, theirs, mixed_o, tin_o, tout_o, tallies, sems):
    copies = [pltpu.make_async_copy(mixed_v, mixed_o.at[0], sems.at[UNITS])]
    copies[0].start()
    for index in [*range(PIECES, UNITS), *range(PIECES)]:
        tallies[index] = votes[index] + theirs[index]
        if index < PIECES:
            target = tin_o.at[:, pl.ds(index * WIDTH, WIDTH)]
        else:
            target = tout_o.at[index - PIECES]
        copies.append(pltpu.make_async_copy(tallies.at[index], target, sems.at[index]))
        copies[-1].start()
    for copy in copies:
        copy.wait()


def shards(patches, cotangent, w_in, w_out, moment_in, moment_out):
    by_piece = (PIECES, WIDTH, FEATURES)
    anywhere = pl.BlockSpec(memory_space=pl.ANY)
    in_vmem = pl.BlockSpec(memory_space=pltpu.VMEM)
    results = pl.pallas_call(
        step_kernel,
        out_shape=(
            pltpu.VMEM((TOKENS, FEATURES), BF16),
            pltpu.VMEM((UNITS, WIDTH, FEATURES), BF16),
            pltpu.VMEM((UNITS, WIDTH, FEATURES), BF16),
        ),
        in_specs=[anywhere] * 6,
        out_specs=(in_vmem,) * 3,
        scratch_shapes=[
            pltpu.VMEM((UNITS, TOKENS, FEATURES), BF16),
            pltpu.VMEM((UNITS, WIDTH, FEATURES), BF16),
            pltpu.VMEM((UNITS, WIDTH, FEATURES), BF16),
            pltpu.VMEM((UNITS, PIECES, TOKENS, WIDTH), BF16),
            pltpu.VMEM((UNITS, 2, TOKENS, WIDTH), F32),
            pltpu.VMEM((UNITS, 2, TOKENS, WIDTH), BF16),
            pltpu.VMEM((UNITS, 4, TOKENS, WIDTH), BF16),
            pltpu.VMEM((UNITS, 2, RING, SUB, WIDTH), BF16),
            pltpu.VMEM((UNITS, 2, RING, SUB, WIDTH), F32),
            pltpu.VMEM((UNITS, 2, SUB, WIDTH), BF16),
            pltpu.VMEM((UNITS, 4, SUB, WIDTH), BF16),
            pltpu.VMEM((BLOCKS, 2, SUB, WIDTH), F32),
            pltpu.VMEM((UNITS, PIECES, RING, SUB, WIDTH), BF16),
            pltpu.VMEM((FEATURES, BLOCKS * TOKENS), BF16),
            pltpu.VMEM((PIECES, WIDTH, BLOCKS * TOKENS), BF16),
            pltpu.VMEM((BLOCKS, TOKENS, FEATURES), F32),
            pltpu.VMEM((BLOCKS, TOKENS, FEATURES), F32),
            pltpu.SemaphoreType.DMA((4 + 2 * PIECES,)),
            pltpu.SemaphoreType.DMA((UNITS,)),
            pltpu.SemaphoreType.DMA((UNITS,)),
            pltpu.SemaphoreType.DMA((4, UNITS)),
            pltpu.SemaphoreType.DMA((4, UNITS)),
            pltpu.SemaphoreType.DMA((4, UNITS)),
            pltpu.SemaphoreType.DMA((5, UNITS)),
            pltpu.SemaphoreType.DMA((BLOCKS,)),
            pltpu.SemaphoreType.DMA((BLOCKS,)),
            pltpu.SemaphoreType.DMA((UNITS,)),
            pltpu.SemaphoreType.DMA((UNITS,)),
        ],
        compiler_params=pltpu.CompilerParams(
            collective_id=0, has_side_effects=True, vmem_limit_bytes=VMEM_LIMIT
        ),
    )(
        patches, cotangent, w_in, w_out.reshape(by_piece), moment_in, moment_out[0].reshape(by_piece),
    )
    mixed, tally_first, tally_second = pl.pallas_call(
        output_kernel,
        out_shape=(
            jax.ShapeDtypeStruct((1, TOKENS, FEATURES), BF16),
            jax.ShapeDtypeStruct((FEATURES, PIECES * WIDTH), BF16),
            jax.ShapeDtypeStruct(by_piece, BF16),
        ),
        in_specs=[in_vmem] * 3,
        out_specs=(anywhere,) * 3,
        scratch_shapes=[
            pltpu.VMEM((UNITS, WIDTH, FEATURES), BF16),
            pltpu.SemaphoreType.DMA((UNITS + 1,)),
        ],
        compiler_params=pltpu.CompilerParams(vmem_limit_bytes=8 * 2**20),
    )(*results)
    return mixed, tally_first, tally_second.reshape(PIECES * WIDTH, FEATURES)


def solution(mesh):
    in_specs = (
        P("rep", "col", "row"),
        P("rep", "col", "row"),
        P("row", "col"),
        P("col", "row"),
        P("rep", "row", "col"),
        P("rep", "col", "row"),
    )
    out_specs = (P("rep", "col", "row"), P("row", "col"), P("col", "row"))
    return jax.shard_map(shards, mesh=mesh, in_specs=in_specs, out_specs=out_specs, check_vma=False)
```

```python
import math

import jax
import jax.numpy as jnp
from jax import lax
from jax.experimental import pallas as pl
from jax.experimental.pallas import tpu as pltpu
from jax.sharding import PartitionSpec as P

MESH = pl.DeviceIdType.MESH
BF16, F32 = jnp.bfloat16, jnp.float32

momentum_decay = 0.9
vote_scale = 0.3

BLOCKS, TOKENS, FEATURES, PIECES, WIDTH = 8, 64, 384, 8, 384
UNITS = 2 * BLOCKS
RING = 4
SUB = TOKENS // RING
LAGS = (0, 2, 5, 7, 10, 13, 16, 21, 26)
VMEM_LIMIT = 50 * 1024 * 1024
TURNS = UNITS + LAGS[-1]


def gelu_value(pre):
    return 0.5 * pre * (1.0 + lax.erf(pre * (1.0 / math.sqrt(2.0))))


def gelu_slope(pre):
    return 0.5 * (1.0 + lax.erf(pre * (1.0 / math.sqrt(2.0)))) + pre * jnp.exp(-0.5 * pre * pre) * (
        1.0 / math.sqrt(2.0 * math.pi)
    )


def unit_at(place):
    moved = jnp.where(place <= BLOCKS, place - 1, place)
    return jnp.where(place == 0, 0, jnp.where(place == 1, BLOCKS, moved))


def token_offset(slot):
    return ((slot + 1) // 2) * ((slot % 2) * 2 - 1)


def step_kernel(
    pat_h, cot_h, win_h, wout_h, min_h, mout_h,
    mixed_v, votes, theirs,
    xs, ws, mom, part, own, t1, r1, summed, total_s, t2, r2, pre_s, act, pat_t, hid_t,
    mpart, mrecv,
    ld, zsend, zrecv, rsend, rrecv, asend, arecv, msend, mrcv, vsend, vrcv,
):
    row, col, rep = lax.axis_index("row"), lax.axis_index("col"), lax.axis_index("rep")
    x, y = row % RING, row // RING
    a = x * (1 - rep) + y * rep
    b = y * (1 - rep) + x * rep

    def peer(a_to, b_to):
        x_to = a_to * (1 - rep) + b_to * rep
        y_to = b_to * (1 - rep) + a_to * rep
        return (y_to * RING + x_to, col, rep)

    ap, am, a2 = (a + 1) % RING, (a + 3) % RING, (a + 2) % RING
    bp, bm, b2 = (b + 1) % RING, (b + 3) % RING, (b + 2) % RING
    to_ap, to_am, to_bp, to_bm = peer(ap, b), peer(am, b), peer(a, bp), peer(a, bm)
    partner = (row, col, 1 - rep)

    def send(src, dst, send_sem, recv_sem, device):
        copy = pltpu.make_async_remote_copy(
            src_ref=src, dst_ref=dst, send_sem=send_sem, recv_sem=recv_sem,
            device_id=device, device_id_type=MESH,
        )
        copy.start()

    def arrived(ref, sem):
        pltpu.make_async_remote_copy(
            src_ref=ref, dst_ref=ref, send_sem=sem, recv_sem=sem, device_id=partner, device_id_type=MESH
        ).wait_recv()

    def departed(ref, sem):
        pltpu.make_async_remote_copy(
            src_ref=ref, dst_ref=ref, send_sem=sem, recv_sem=sem, device_id=partner, device_id_type=MESH
        ).wait_send()

    def products(q, second):
        tokens = xs[q]
        for block in (a2, ap, am, a):
            if second:
                pair = ws[pl.ds(PIECES + 2 * block, 2)].reshape(2 * WIDTH, FEATURES)
                term = lax.dot_general(tokens, pair, (((1,), (1,)), ((), ())), preferred_element_type=F32)
            else:
                pair = jnp.concatenate([ws[2 * block], ws[2 * block + 1]], axis=1)
                term = jnp.dot(tokens, pair, preferred_element_type=F32)
            for h in range(2):
                half = term[:, h * WIDTH : (h + 1) * WIDTH]
                if block is a:
                    own[q, h] = half
                else:
                    part[q, 2 * block + h] = half.astype(BF16)

    load_x = [
        pltpu.make_async_copy(pat_h.at[0], xs.at[0], ld.at[0]),
        pltpu.make_async_copy(cot_h.at[0], xs.at[BLOCKS], ld.at[1]),
    ]
    load_win = [
        pltpu.make_async_copy(win_h.at[:, pl.ds(p * WIDTH, WIDTH)], ws.at[p], ld.at[4 + p]) for p in range(PIECES)
    ]
    load_wout = pltpu.make_async_copy(wout_h, ws.at[pl.ds(PIECES, PIECES)], ld.at[2])
    load_mout = pltpu.make_async_copy(mout_h, mom.at[pl.ds(PIECES, PIECES)], ld.at[3])
    load_min = [
        pltpu.make_async_copy(min_h.at[0, :, pl.ds(p * WIDTH, WIDTH)], mom.at[p], ld.at[4 + PIECES + p])
        for p in range(PIECES)
    ]
    barrier = pltpu.get_barrier_semaphore()
    below, above = (row, (col + BLOCKS - 1) % BLOCKS, rep), (row, (col + 1) % BLOCKS, rep)
    peers = [to_ap, to_am, to_bp, to_bm, partner, below, above]
    for device in peers:
        pl.semaphore_signal(barrier, inc=1, device_id=device, device_id_type=MESH)
    for copy in load_x + load_win + [load_wout]:
        copy.start()
    for copy in load_x + load_win:
        copy.wait()
    products(0, False)
    pl.semaphore_wait(barrier, len(peers))

    for base in (0, BLOCKS):
        send(xs.at[base], xs.at[base + 1], zsend.at[base + 1], zrecv.at[base + 1], below)
        send(xs.at[base], xs.at[base + 2], zsend.at[base + 2], zrecv.at[base + 2], above)

    load_wout.wait()
    for copy in load_min + [load_mout]:
        copy.start()

    def prepare(q):
        @pl.when(q % BLOCKS != 0)
        def _():
            arrived(xs.at[q], zrecv.at[q])

        @pl.when((q % BLOCKS >= 1) & (q % BLOCKS < BLOCKS - 2))
        def _():
            onward = (row, (col + BLOCKS + 1 - 2 * (q % 2)) % BLOCKS, rep)
            send(xs.at[q], xs.at[q + 2], zsend.at[q + 2], zrecv.at[q + 2], onward)

        @pl.when(q < BLOCKS)
        def _():
            products(q, False)

        @pl.when(q >= BLOCKS)
        def _():
            products(q, True)

    def reduce_start(q):
        send(part.at[q, 2 * a2], t1.at[q, 0], rsend.at[0, q], rrecv.at[0, q], to_ap)
        send(part.at[q, 2 * a2 + 1], t1.at[q, 1], rsend.at[0, q], rrecv.at[0, q], to_am)
        send(part.at[q, 2 * ap + 1], r1.at[q, 1], rsend.at[0, q], rrecv.at[1, q], to_ap)
        send(part.at[q, 2 * am], r1.at[q, 2], rsend.at[0, q], rrecv.at[1, q], to_am)

    def reduce_relay(q):
        arrived(t1.at[q], rrecv.at[0, q])
        part[q, 2 * ap] = (part[q, 2 * ap].astype(F32) + t1[q, 0].astype(F32)).astype(BF16)
        part[q, 2 * am + 1] = (part[q, 2 * am + 1].astype(F32) + t1[q, 1].astype(F32)).astype(BF16)
        send(part.at[q, 2 * ap], r1.at[q, 0], rsend.at[1, q], rrecv.at[1, q], to_ap)
        send(part.at[q, 2 * am + 1], r1.at[q, 3], rsend.at[1, q], rrecv.at[1, q], to_am)

    def second_start(q):
        arrived(r1.at[q], rrecv.at[1, q])
        for h in range(2):
            total = own[q, h] + r1[q, h].astype(F32) + r1[q, 2 + h].astype(F32)
            total = total.reshape(RING, SUB, WIDTH)
            total_s[q, h] = total
            summed[q, h] = total.astype(BF16)
        send(summed.at[q, 0, b2], t2.at[q, 0], rsend.at[2, q], rrecv.at[2, q], to_bp)
        send(summed.at[q, 1, b2], t2.at[q, 1], rsend.at[2, q], rrecv.at[2, q], to_bm)
        send(summed.at[q, 1, bp], r2.at[q, 1], rsend.at[2, q], rrecv.at[3, q], to_bp)
        send(summed.at[q, 0, bm], r2.at[q, 2], rsend.at[2, q], rrecv.at[3, q], to_bm)

    def second_relay(q):
        arrived(t2.at[q], rrecv.at[2, q])
        summed[q, 0, bp] = (summed[q, 0, bp].astype(F32) + t2[q, 0].astype(F32)).astype(BF16)
        summed[q, 1, bm] = (summed[q, 1, bm].astype(F32) + t2[q, 1].astype(F32)).astype(BF16)
        send(summed.at[q, 0, bp], r2.at[q, 0], rsend.at[3, q], rrecv.at[3, q], to_bp)
        send(summed.at[q, 1, bm], r2.at[q, 3], rsend.at[3, q], rrecv.at[3, q], to_bm)

    def activate(q):
        arrived(r2.at[q], rrecv.at[3, q])
        totals = [
            total_s[q, h, b] + r2[q, h].astype(F32) + r2[q, 2 + h].astype(F32) for h in range(2)
        ]

        @pl.when(q < BLOCKS)
        def _():
            for h in range(2):
                pre_s[q, h] = totals[h]
                act[q, 2 * a + h, b] = gelu_value(totals[h]).astype(BF16)

        @pl.when(q >= BLOCKS)
        def _():
            for h in range(2):
                slope = gelu_slope(pre_s[q - BLOCKS, h])
                act[q, 2 * a + h, b] = (totals[h] * slope).astype(BF16)

        mine = act.at[q, pl.ds(2 * a, 2), b]
        send(mine, mine, asend.at[0, q], arecv.at[0, q], to_bp)
        send(mine, mine, asend.at[0, q], arecv.at[0, q], to_bm)

    def second_spread(q):
        arrived(part.at[q, 0], arecv.at[0, q])
        ahead, behind = act.at[q, 2 * a, bm], act.at[q, 2 * a + 1, bp]
        send(ahead, ahead, asend.at[1, q], arecv.at[1, q], to_bp)
        send(behind, behind, asend.at[1, q], arecv.at[1, q], to_bm)

    def first_spread(q):
        arrived(t2.at[q], arecv.at[1, q])
        near, far = act.at[q, 2 * a], act.at[q, 2 * a + 1]
        send(near, near, asend.at[2, q], arecv.at[2, q], to_ap)
        send(far, far, asend.at[2, q], arecv.at[2, q], to_am)
        send(far, far, asend.at[2, q], arecv.at[4, q], to_ap)
        send(near, near, asend.at[2, q], arecv.at[4, q], to_am)

    def first_relay(q):
        arrived(t1.at[q], arecv.at[2, q])
        ahead, behind = act.at[q, 2 * am], act.at[q, 2 * ap + 1]
        send(ahead, ahead, asend.at[3, q], arecv.at[3, q], to_ap)
        send(behind, behind, asend.at[3, q], arecv.at[3, q], to_am)

    def complete(q):
        arrived(t1.at[q], arecv.at[4, q])
        arrived(t1.at[q], arecv.at[3, q])

        @pl.when(q < BLOCKS)
        def _():
            total = jnp.zeros((TOKENS, FEATURES), F32)
            for p in range(PIECES):
                total += jnp.dot(
                    act[q, p].reshape(TOKENS, WIDTH), ws[PIECES + p], preferred_element_type=F32
                )

            mpart[q] = total

            @pl.when(q % 2 == 1)
            def _():
                rows = pl.ds(pl.multiple_of((q - 1) * TOKENS, 2 * TOKENS), 2 * TOKENS)
                for p in range(PIECES):
                    hid_t[p, :, rows] = act[pl.ds(q - 1, 2), p].reshape(2 * TOKENS, WIDTH).T

            @pl.when(q > 0)
            def _():
                target = (row, (col + token_offset(q) + BLOCKS) % BLOCKS, rep)
                send(mpart.at[q], mrecv.at[q], msend.at[q], mrcv.at[q], target)

    grad_factor = (1.0 - momentum_decay) / vote_scale / math.sqrt(BLOCKS * TOKENS)
    moment_factor = momentum_decay / vote_scale

    def vote(grad, index):
        moved = moment_factor * mom[index].astype(F32) + grad_factor * grad
        votes[index] = jnp.tanh(moved).astype(BF16)
        send(votes.at[index], theirs.at[index], vsend.at[index], vrcv.at[index], partner)

    def vote_second(p):
        cotangent = xs[pl.ds(BLOCKS, BLOCKS)].reshape(BLOCKS * TOKENS, FEATURES)
        grad = jnp.dot(hid_t[p], cotangent, preferred_element_type=F32)
        vote(grad, PIECES + p)

    def vote_first(block):
        pieces = [act[pl.ds(BLOCKS, BLOCKS), 2 * block + h].reshape(BLOCKS * TOKENS, WIDTH) for h in range(2)]
        grad = jnp.dot(pat_t[...], jnp.concatenate(pieces, axis=1), preferred_element_type=F32)
        for h in range(2):
            vote(grad[:, h * WIDTH : (h + 1) * WIDTH], 2 * block + h)

    stages = (
        (LAGS[0], reduce_start), (LAGS[1], reduce_relay), (LAGS[7], first_relay), (LAGS[6], first_spread),
        (LAGS[2], second_start), (LAGS[3], second_relay), (LAGS[4], activate), (LAGS[5], second_spread),
    )

    def turn(i, carry):
        for lag, stage in stages:

            @pl.when((i >= lag) & (i < UNITS + lag))
            def _(lag=lag, stage=stage):
                stage(unit_at(i - lag))

        @pl.when(i < UNITS - 1)
        def _():
            prepare(unit_at(i + 1))

        @pl.when(i == TURNS - BLOCKS)
        def _():
            load_mout.wait()
            pat_t[...] = xs[pl.ds(0, BLOCKS)].reshape(BLOCKS * TOKENS, FEATURES).T

        @pl.when(i > TURNS - BLOCKS)
        def _():
            vote_second(i - (TURNS - BLOCKS) - 1)

        @pl.when(i == TURNS - 1)
        def _():
            vote_second(PIECES - 1)

        @pl.when((i >= LAGS[8]) & (i < UNITS + LAGS[8]))
        def _():
            complete(unit_at(i - LAGS[8]))

        return carry

    lax.fori_loop(0, TURNS, turn, 0)

    for copy in load_min:
        copy.wait()

    def first_turn(p, carry):
        vote_first(p)
        return carry

    lax.fori_loop(0, PIECES // 2, first_turn, 0)

    total = mpart[0]
    for slot in range(1, BLOCKS):
        arrived(mrecv.at[slot], mrcv.at[slot])
        total += mrecv[slot]
    mixed_v[...] = total.astype(BF16)

    def drain(q, carry):
        departed(part.at[q, pl.ds(0, 4)], rsend.at[0, q])
        departed(part.at[q, pl.ds(0, 2)], rsend.at[1, q])
        departed(summed.at[q, 0], rsend.at[2, q])
        departed(t2.at[q], rsend.at[3, q])
        departed(summed.at[q, 0], asend.at[0, q])
        departed(t2.at[q], asend.at[1, q])
        departed(part.at[q, pl.ds(0, 4)], asend.at[2, q])
        departed(part.at[q, pl.ds(0, 2)], asend.at[3, q])
        departed(votes.at[q], vsend.at[q])

        @pl.when(q % BLOCKS != 0)
        def _():
            departed(xs.at[q], zsend.at[q])

        return carry

    lax.fori_loop(0, UNITS, drain, 0)
    for slot in range(1, BLOCKS):
        departed(mpart.at[slot], msend.at[slot])

    def theirs_in(q, carry):
        arrived(theirs.at[UNITS - 1 - q], vrcv.at[UNITS - 1 - q])
        return carry

    lax.fori_loop(0, UNITS, theirs_in, 0)


def output_kernel(mixed_v, votes, theirs, mixed_o, tin_o, tout_o, tallies, sems):
    copies = [pltpu.make_async_copy(mixed_v, mixed_o.at[0], sems.at[UNITS])]
    copies[0].start()
    for index in [*range(PIECES, UNITS), *range(PIECES)]:
        tallies[index] = votes[index] + theirs[index]
        if index < PIECES:
            target = tin_o.at[:, pl.ds(index * WIDTH, WIDTH)]
        else:
            target = tout_o.at[index - PIECES]
        copies.append(pltpu.make_async_copy(tallies.at[index], target, sems.at[index]))
        copies[-1].start()
    for copy in copies:
        copy.wait()


def shards(patches, cotangent, w_in, w_out, moment_in, moment_out):
    by_piece = (PIECES, WIDTH, FEATURES)
    anywhere = pl.BlockSpec(memory_space=pl.ANY)
    in_vmem = pl.BlockSpec(memory_space=pltpu.VMEM)
    results = pl.pallas_call(
        step_kernel,
        out_shape=(
            pltpu.VMEM((TOKENS, FEATURES), BF16),
            pltpu.VMEM((UNITS, WIDTH, FEATURES), BF16),
            pltpu.VMEM((UNITS, WIDTH, FEATURES), BF16),
        ),
        in_specs=[anywhere] * 6,
        out_specs=(in_vmem,) * 3,
        scratch_shapes=[
            pltpu.VMEM((UNITS, TOKENS, FEATURES), BF16),
            pltpu.VMEM((UNITS, WIDTH, FEATURES), BF16),
            pltpu.VMEM((UNITS, WIDTH, FEATURES), BF16),
            pltpu.VMEM((UNITS, PIECES, TOKENS, WIDTH), BF16),
            pltpu.VMEM((UNITS, 2, TOKENS, WIDTH), F32),
            pltpu.VMEM((UNITS, 2, TOKENS, WIDTH), BF16),
            pltpu.VMEM((UNITS, 4, TOKENS, WIDTH), BF16),
            pltpu.VMEM((UNITS, 2, RING, SUB, WIDTH), BF16),
            pltpu.VMEM((UNITS, 2, RING, SUB, WIDTH), F32),
            pltpu.VMEM((UNITS, 2, SUB, WIDTH), BF16),
            pltpu.VMEM((UNITS, 4, SUB, WIDTH), BF16),
            pltpu.VMEM((BLOCKS, 2, SUB, WIDTH), F32),
            pltpu.VMEM((UNITS, PIECES, RING, SUB, WIDTH), BF16),
            pltpu.VMEM((FEATURES, BLOCKS * TOKENS), BF16),
            pltpu.VMEM((PIECES, WIDTH, BLOCKS * TOKENS), BF16),
            pltpu.VMEM((BLOCKS, TOKENS, FEATURES), F32),
            pltpu.VMEM((BLOCKS, TOKENS, FEATURES), F32),
            pltpu.SemaphoreType.DMA((4 + 2 * PIECES,)),
            pltpu.SemaphoreType.DMA((UNITS,)),
            pltpu.SemaphoreType.DMA((UNITS,)),
            pltpu.SemaphoreType.DMA((4, UNITS)),
            pltpu.SemaphoreType.DMA((4, UNITS)),
            pltpu.SemaphoreType.DMA((4, UNITS)),
            pltpu.SemaphoreType.DMA((5, UNITS)),
            pltpu.SemaphoreType.DMA((BLOCKS,)),
            pltpu.SemaphoreType.DMA((BLOCKS,)),
            pltpu.SemaphoreType.DMA((UNITS,)),
            pltpu.SemaphoreType.DMA((UNITS,)),
        ],
        compiler_params=pltpu.CompilerParams(
            collective_id=0, has_side_effects=True, vmem_limit_bytes=VMEM_LIMIT
        ),
    )(
        patches, cotangent, w_in, w_out.reshape(by_piece), moment_in, moment_out[0].reshape(by_piece),
    )
    mixed, tally_first, tally_second = pl.pallas_call(
        output_kernel,
        out_shape=(
            jax.ShapeDtypeStruct((1, TOKENS, FEATURES), BF16),
            jax.ShapeDtypeStruct((FEATURES, PIECES * WIDTH), BF16),
            jax.ShapeDtypeStruct(by_piece, BF16),
        ),
        in_specs=[in_vmem] * 3,
        out_specs=(anywhere,) * 3,
        scratch_shapes=[
            pltpu.VMEM((UNITS, WIDTH, FEATURES), BF16),
            pltpu.SemaphoreType.DMA((UNITS + 1,)),
        ],
        compiler_params=pltpu.CompilerParams(vmem_limit_bytes=8 * 2**20),
    )(*results)
    return mixed, tally_first, tally_second.reshape(PIECES * WIDTH, FEATURES)


def solution(mesh):
    in_specs = (
        P("rep", "col", "row"),
        P("rep", "col", "row"),
        P("row", "col"),
        P("col", "row"),
        P("rep", "row", "col"),
        P("rep", "col", "row"),
    )
    out_specs = (P("rep", "col", "row"), P("row", "col"), P("col", "row"))
    return jax.shard_map(shards, mesh=mesh, in_specs=in_specs, out_specs=out_specs, check_vma=False)
```
